256 devices in a mesh: kf: 64 (over z, y, core), kc: 4 (over x).
Axes of the slice: x: 4, y: 4, z: 8, core: 2. Of those that a mesh axis runs over, the one named last changes fastest.
Arguments:
- kernel_coarse: bfloat16 [2048, 2048], P('kf'), may hold values from -6 to 6
- coefficients: bfloat16 [1024, 256], P(('kf', 'kc')), may hold values from -1.5 to 1.5
- nearest: int32 [1024], replicated, may hold values from 0 to 127
Outputs:
- kernel_fine: bfloat16 [16384, 16384], P('kf', 'kc')
The draws below stay inside these ranges and needn't reach their ends.
All inputs are finite; a program needn't handle non-finite values.
Results may differ from the reference program's by a relative error of at most 0.0049.
Values may be sent and summed in bfloat16 or wider, within the bound.
No kernel may reach another device: no remote copies, remote signals or barrier semaphores. Data moves between devices by JAX's collectives and lax.ppermute only.
A program may use at most 64 MiB of HBM per device.

```python
import jax
import jax.numpy as jnp
from jax import lax

P_SIZE = 16
FK_DEV = 16
FINE = 1024
COARSE = 128
N_KF = 64


def touch_ends(entries, stream_key, low, largest):
    index_at = [jax.random.randint(jax.random.fold_in(stream_key, axis), (), 0, length) for axis, length in enumerate(entries.shape)]
    widest = entries.shape.index(max(entries.shape))
    neighbour = index_at[:widest] + [(index_at[widest] + 1) % entries.shape[widest]] + index_at[widest + 1:]
    return entries.at[tuple(index_at)].set(low).at[tuple(neighbour)].set(largest)


def steps_of(own_key, shape, cuts, least, top_value):
    loudness, own = 1.0, jax.random.fold_in(own_key, 6)
    for position, blocks in cuts:
        draws = jnp.exp(jax.random.uniform(jax.random.fold_in(own, position), (blocks,), jnp.float32, least / len(cuts), top_value / len(cuts)))
        loudness = loudness * jnp.repeat(draws, shape[position] // blocks).reshape([-1 if axis == position else 1 for axis in range(len(shape))])
    return loudness


def gaussian(stream_key, shape, spread, reach, shards=(), kind=jnp.bfloat16):
    array = spread * jax.random.normal(stream_key, shape, jnp.float32)
    if shards:
        array = array * steps_of(stream_key, shape, shards, -0.22, 0.18)
    return jnp.clip(array, -reach, reach).astype(kind)


def setup_inputs(seed: int = 0) -> dict:
    streams_of = jax.random.split(jax.random.key(seed), 4)
    return {
        "kernel_coarse": gaussian(streams_of[0], (COARSE * P_SIZE, COARSE * P_SIZE), 1.0, 6.0, ((0, 64),)),
        "coefficients": gaussian(streams_of[1], (FINE, P_SIZE * P_SIZE), P_SIZE ** -0.5, 1.5, ((0, 256),)),
        "nearest": touch_ends(jax.random.randint(streams_of[2], (FINE,), 0, COARSE), jax.random.fold_in(streams_of[2], 1), 0, COARSE - 1).astype(jnp.int32),
    }


def reference(kernel_coarse, coefficients, nearest):
    offsets = jnp.arange(P_SIZE, dtype=jnp.int32)
    columns = (nearest[:, None] * P_SIZE + offsets[None, :]).reshape(-1)
    coef_all = coefficients.reshape(FINE, P_SIZE, P_SIZE).astype(jnp.float32)
    gathered = jnp.take(kernel_coarse, columns, axis=1).astype(jnp.float32).reshape(COARSE * P_SIZE, FINE, P_SIZE)
    rotated = jnp.einsum("ckn,kan->cka", gathered, coef_all).astype(jnp.bfloat16).reshape(COARSE, P_SIZE, FINE * P_SIZE)

    def expand(block_index):
        col_points = lax.dynamic_slice_in_dim(nearest, block_index * FK_DEV, FK_DEV)
        coef_block = lax.dynamic_slice_in_dim(coef_all, block_index * FK_DEV, FK_DEV, 0)
        picked = jnp.take(rotated, col_points, axis=0).astype(jnp.float32)
        return jnp.einsum("jnr,jbn->jbr", picked, coef_block).astype(jnp.bfloat16)

    blocks = lax.map(expand, jnp.arange(N_KF, dtype=jnp.int32))
    return blocks.reshape(FINE * P_SIZE, FINE * P_SIZE).T
```

```python
import jax
import jax.numpy as jnp
from jax import lax
from jax.experimental import pallas as pl
from jax.experimental.pallas import tpu as pltpu
from jax.sharding import Mesh
from jax.sharding import PartitionSpec as P

KF = ("kf_0", "kf_1", "kf_2")
ZY = ("kf_0", "kf_1")
KF_KC = ("kf_0", "kf_1", "kf_2", "kc")
LANES = 128
PAIRS = 16
POINTS = 4
PEERS = 32


def iota(shape, dim):
    return lax.broadcasted_iota(jnp.int32, shape, dim)


def spread_rows(coef):
    group = iota((PAIRS, LANES), 1) // PAIRS
    row = iota((PAIRS, LANES), 0)
    keep = group == row % 8
    low = row < 8
    pieces = []
    for p in range(coef.shape[0]):
        first = jnp.broadcast_to(coef[p : p + 1, :LANES], (PAIRS, LANES))
        second = jnp.broadcast_to(coef[p : p + 1, LANES:], (PAIRS, LANES))
        pieces.append(jnp.where(keep, jnp.where(low, first, second), 0.0))
    return jnp.concatenate(pieces, axis=0).astype(jnp.bfloat16)


def repeated(width):
    same = iota((LANES, width), 0) % PAIRS == iota((LANES, width), 1) % PAIRS
    return jnp.where(same, 1.0, 0.0).astype(jnp.bfloat16)


def pack_kernel(near, own, other, coef_own, coef_other, out, blocks):
    kc = lax.axis_index("kc")
    core = lax.axis_index("kf_2")
    for b in range(16):
        cut = slice(b * LANES, (b + 1) * LANES)
        blocks[core, b] = own[:, cut].astype(jnp.float32)
        blocks[1 - core, b] = other[:, cut].astype(jnp.float32)
    a = coef_own[...].astype(jnp.float32)
    o = coef_other[...].astype(jnp.float32)
    first = jnp.where(core == 0, a, o)
    second = jnp.where(core == 0, o, a)
    coef = jnp.concatenate(
        [first[:, :LANES], first[:, LANES:], second[:, :LANES], second[:, LANES:]], axis=0
    ).astype(jnp.bfloat16)
    group = iota((PAIRS, LANES), 1) // PAIRS
    base = 16 * core + 4 * kc

    def body(d, carry):
        for h in range(2):
            tile = jnp.zeros((PAIRS, LANES), jnp.float32)
            for j in range(POINTS):
                c = near[32 * d + base + j]
                for lo in range(2):
                    at = lo * POINTS + j
                    piece = blocks[h, c // 8, lo * PAIRS : (lo + 1) * PAIRS, :]
                    turned = pltpu.roll(piece, ((at - c % 8) % 8) * PAIRS, 1)
                    tile = jnp.where(group == at, turned, tile)
            out[d, h * PAIRS : (h + 1) * PAIRS, :] = tile.astype(jnp.bfloat16)
        out[d, 2 * PAIRS :, :] = coef
        return carry

    lax.fori_loop(0, PEERS, body, 0)


def final_kernel(near, mine, left, right, far_a, far_b, coef_cols, rows_0, rows_l, rows_r, rows_f, out, turn):
    kc = lax.axis_index("kc")
    t = pl.program_id(0)

    @pl.when(t == 0)
    def _():
        keep = iota((POINTS * PAIRS, LANES), 1) // PAIRS % POINTS == iota((POINTS * PAIRS, LANES), 0) // PAIRS
        for i, ref in enumerate((rows_0, rows_l, rows_r, rows_f)):
            wide = jnp.dot(
                spread_rows(ref[...].astype(jnp.float32)), repeated(LANES), preferred_element_type=jnp.float32
            )
            turn[i] = jnp.where(keep, wide, 0.0).astype(jnp.bfloat16)

    z_low, y, core = t // 8, t // 2 % 4, t % 2
    spread = []
    for x in range(4):
        chunk = coef_cols[(z_low * 4 + x) * 4 + y, pl.ds(core * 8, 8), :].astype(jnp.float32)
        spread.append(spread_rows(jnp.concatenate([chunk[:POINTS], chunk[POINTS:]], axis=1)))
    wide = jnp.dot(jnp.concatenate(spread, axis=0), repeated(256), preferred_element_type=jnp.float32)
    diag = iota((256, 256), 0) // PAIRS == iota((256, 256), 1) // PAIRS
    cols = jnp.where(diag, wide, 0.0).astype(jnp.bfloat16)

    half = iota((PAIRS, LANES), 1) // 64
    picks = [[], [], [], []]
    for i in range(16):
        c = near[256 * kc + 16 * t + i]
        zy = c // 4
        at = pl.multiple_of((c // 2 % 2) * PAIRS, PAIRS)
        keep = half == c % 2
        far = jnp.where(
            zy < PEERS // 2,
            far_a[jnp.minimum(zy, PEERS // 2 - 1), pl.ds(at, PAIRS), :],
            far_b[jnp.maximum(zy - PEERS // 2, 0), pl.ds(at, PAIRS), :],
        )
        for n, block in enumerate((mine[zy, pl.ds(at, PAIRS), :], left[zy, pl.ds(at, PAIRS), :], right[zy, pl.ds(at, PAIRS), :], far)):
            picks[n].append(jnp.where(keep, block, jnp.zeros_like(block)))
    for n, step in enumerate((0, 3, 1, 2)):
        block = jnp.concatenate(picks[n], axis=0)
        turned = lax.dot_general(turn[n], block, (((1,), (1,)), ((), ())), preferred_element_type=jnp.float32)
        result = lax.dot_general(
            turned.astype(jnp.bfloat16), cols, (((1,), (1,)), ((), ())), preferred_element_type=jnp.float32
        )
        at = pl.multiple_of((kc + step) % 4 * 64, 64)
        out[pl.ds(at, 64), :] = result.astype(jnp.bfloat16)


def shift(value, by):
    return lax.ppermute(value, "kc", [(i, (i + by) % 4) for i in range(4)])


def spread_coefficients(swap_core):
    pairs = []
    for z in range(8):
        for y in range(4):
            for c in range(2):
                for x in range(4):
                    new_c = 1 - c if swap_core else c
                    source = ((z * 4 + y) * 2 + c) * 4 + x
                    target = ((((z % 2) * 4 + x) * 4 + y) * 2 + new_c) * 4 + z // 2
                    pairs.append((source, target))
    return pairs


def shards(kernel_coarse, coefficients, nearest):
    vmem = pl.BlockSpec(memory_space=pltpu.VMEM)
    smem = pl.BlockSpec(memory_space=pltpu.SMEM)
    other = lax.ppermute(kernel_coarse, "kf_2", [(0, 1), (1, 0)])
    coef_own = lax.ppermute(coefficients, KF_KC, spread_coefficients(False))
    coef_other = lax.ppermute(coefficients, KF_KC, spread_coefficients(True))
    outgoing = pl.pallas_call(
        pack_kernel,
        out_shape=jax.ShapeDtypeStruct((PEERS, 48, LANES), jnp.bfloat16),
        in_specs=[smem, vmem, vmem, vmem, vmem],
        out_specs=vmem,
        scratch_shapes=[pltpu.VMEM((2, 16, 32, LANES), jnp.float32)],
        compiler_params=pltpu.CompilerParams(vmem_limit_bytes=8 << 20),
        cost_estimate=pl.CostEstimate(flops=4000000, bytes_accessed=650000, transcendentals=0),
    )(nearest, kernel_coarse, other, coef_own, coef_other)
    received = lax.all_to_all(outgoing, ZY, split_axis=0, concat_axis=0, tiled=True)
    mine = received[:, :32]
    coef_cols = received[:, 32:]
    left = shift(mine, 1)
    right = shift(mine, -1)
    far_a = shift(left[: PEERS // 2], 1)
    far_b = shift(right[PEERS // 2 :], -1)
    rows_l, rows_r, rows_f = shift(coefficients, 1), shift(coefficients, -1), shift(coefficients, 2)
    return pl.pallas_call(
        final_kernel,
        grid=(16,),
        out_shape=jax.ShapeDtypeStruct((256, 4096), jnp.bfloat16),
        in_specs=[smem] + [vmem] * 10,
        out_specs=pl.BlockSpec((256, 256), lambda t: (0, t)),
        scratch_shapes=[pltpu.VMEM((4, 64, LANES), jnp.bfloat16)],
        compiler_params=pltpu.CompilerParams(vmem_limit_bytes=8 << 20),
        cost_estimate=pl.CostEstimate(flops=20000000, bytes_accessed=3400000, transcendentals=0),
    )(nearest, mine, left, right, far_a, far_b, coef_cols, coefficients, rows_l, rows_r, rows_f)


def solution(mesh):
    split = Mesh(mesh.devices.reshape(8, 4, 2, mesh.shape["kc"]), KF_KC)
    return jax.shard_map(
        shards,
        mesh=split,
        in_specs=(P(KF, None), P(KF_KC, None), P()),
        out_specs=P(KF, "kc"),
        check_vma=False,
    )
```

```python
import jax
import jax.numpy as jnp
from jax import lax
from jax.experimental import pallas as pl
from jax.experimental.pallas import tpu as pltpu
from jax.sharding import Mesh
from jax.sharding import PartitionSpec as P

KF = ("kf_0", "kf_1", "kf_2")
ZY = ("kf_0", "kf_1")
KF_KC = ("kf_0", "kf_1", "kf_2", "kc")
LANES = 128
PAIRS = 16
POINTS = 4
PEERS = 32
BF16 = jnp.bfloat16
F32 = jnp.float32
VMEM = pl.BlockSpec(memory_space=pltpu.VMEM)
SMEM = pl.BlockSpec(memory_space=pltpu.SMEM)
ANY = pl.BlockSpec(memory_space=pl.ANY)


def iota(shape, dim):
    return lax.broadcasted_iota(jnp.int32, shape, dim)


def dot_t(a, b):
    return lax.dot_general(a, b, (((1,), (1,)), ((), ())), preferred_element_type=F32)


def pack_rows(near, rows, out, copies, at_row):
    kc = lax.axis_index("kc")
    core = lax.axis_index("kf_2")
    for b in range(16):
        block = rows[:, b * LANES : (b + 1) * LANES].astype(F32)
        for s in range(8):
            turned = pltpu.roll(block, s * PAIRS, 1) if s else block
            copies[s, b] = turned.astype(BF16)
    group = iota((PAIRS, LANES), 1) // PAIRS
    base = 16 * core + 4 * kc

    def body(d, carry):
        tile = None
        for j in range(POINTS):
            c = near[32 * d + base + j]
            for lo in range(2):
                at = lo * POINTS + j
                piece = copies[(at - c) & 7, c >> 3, lo * PAIRS : (lo + 1) * PAIRS, :]
                tile = piece if tile is None else jnp.where(group == at, piece, tile)
        out[d, pl.ds(at_row, PAIRS), :] = tile
        return carry

    lax.fori_loop(0, PEERS, body, 0, unroll=4)


def pack_own_kernel(near, own, out, copies):
    pack_rows(near, own, out, copies, pl.multiple_of(lax.axis_index("kf_2") * PAIRS, PAIRS))


def pack_other_kernel(near, other, coef_own, coef_other, half_packed, out, copies):
    core = lax.axis_index("kf_2")
    pack_rows(near, other, out, copies, pl.multiple_of((1 - core) * PAIRS, PAIRS))
    a = coef_own[...].astype(F32)
    o = coef_other[...].astype(F32)
    first = jnp.where(core == 0, a, o)
    second = jnp.where(core == 0, o, a)
    coef = jnp.concatenate(
        [first[:, :LANES], first[:, LANES:], second[:, :LANES], second[:, LANES:]], axis=0
    ).astype(BF16)
    for d in range(PEERS):
        out[d, 2 * PAIRS :, :] = coef


def split_kernel(received, coef_own, up, down, across):
    kc = lax.axis_index("kc")
    mine = coef_own[...].astype(F32)
    mine = jnp.concatenate([mine[:, :LANES], mine[:, LANES:]], axis=0)
    mine = jnp.concatenate([mine, jnp.zeros_like(mine)], axis=0).astype(BF16)
    for zy in range(PEERS):
        for h in range(2):
            block = received[zy, h * PAIRS : (h + 1) * PAIRS, :]
            up[2 * zy + h] = block
            down[2 * zy + h] = block
    for step, target, at in ((1, up, 64), (3, down, 64), (2, across, 0)):
        first = (kc + step) % 4 * 8
        for p in range(8):
            target[at + p] = received[first + p, 2 * PAIRS :, :]
        target[at + 8] = mine


def spread(row_of, count):
    keep = iota((8, LANES), 1) // PAIRS == iota((8, LANES), 0)
    pieces = []
    for p in range(count):
        for half in range(2):
            pieces.append(jnp.where(keep, jnp.broadcast_to(row_of(p, half), (8, LANES)), 0.0))
    return jnp.concatenate(pieces, axis=0).astype(BF16)


def repeat_matrix():
    same = iota((LANES, LANES), 0) % PAIRS == iota((LANES, LANES), 1) % PAIRS
    return jnp.where(same, 1.0, 0.0).astype(BF16)


def set_halves(halves):
    low = iota((PAIRS, LANES), 1) < 64
    halves[0] = jnp.where(low, 1.0, 0.0).astype(BF16)
    halves[1] = jnp.where(low, 0.0, 1.0).astype(BF16)


def rotate_points(near, halves, first, sources):
    picks = [[] for _ in sources]
    for i in range(8):
        c = near[first + i]
        keep = halves[c & 1]
        for n, (blocks, _) in enumerate(sources):
            picks[n].append(blocks[c >> 1] * keep)
    return [dot_t(turn, jnp.concatenate(p, axis=0)).astype(BF16) for p, (_, turn) in zip(picks, sources)]


def middle_kernel(near, received, mine, left, right, far_coef, out, cols, turn_far, pieces, turns, halves, result, sem):
    kc = lax.axis_index("kc")
    set_halves(halves)
    repeat = repeat_matrix()
    for p in range(8):
        pieces[kc, p] = received[kc * 8 + p, 2 * PAIRS :, :].astype(F32)
        pieces[(kc + 3) % 4, p] = left[64 + p].astype(F32)
        pieces[(kc + 1) % 4, p] = right[64 + p].astype(F32)
        pieces[(kc + 2) % 4, p] = far_coef[p].astype(F32)
    own_group = iota((64, LANES), 1) // PAIRS % POINTS == iota((64, LANES), 0) // PAIRS
    for n, row in enumerate((mine[72], left[72], right[72], far_coef[8])):
        row = row.astype(F32)
        wide = jnp.dot(
            spread(lambda p, half: row[half * POINTS + p : half * POINTS + p + 1], POINTS),
            repeat,
            preferred_element_type=F32,
        )
        value = jnp.where(own_group, wide, 0.0).astype(BF16)
        if n < 3:
            turns[n] = value
        else:
            turn_far[...] = value
    diag = iota((LANES, LANES), 0) // PAIRS == iota((LANES, LANES), 1) // PAIRS

    def copy(n, v):
        row = pl.multiple_of((kc + (0, 3, 1)[n]) % 4 * 64, 64)
        at = pl.ds(pl.multiple_of(v * 512, 512), 512)
        return pltpu.make_async_copy(result.at[n, :, at], out.at[pl.ds(row, 64), at], sem.at[n, v])

    def body(v, carry):
        for h in range(2):
            for par in range(2):
                u = v * 4 + h * 2 + par

                def row_of(p, half):
                    r = h * 8 + half * POINTS + p % POINTS
                    return pieces[par * 2 + p // POINTS, v, r : r + 1, :]

                wide = jnp.dot(spread(row_of, 8), repeat, preferred_element_type=F32)
                block = jnp.where(diag, wide, 0.0).astype(BF16)
                cols[u] = block
                turned = rotate_points(
                    near, halves, 256 * kc + 8 * u, ((mine, turns[0]), (left, turns[1]), (right, turns[2]))
                )
                at = pl.ds(pl.multiple_of(u * LANES, LANES), LANES)
                for n in range(3):
                    result[n, :, at] = dot_t(turned[n], block).astype(BF16)
        for n in range(3):
            copy(n, v).start()
        return carry

    lax.fori_loop(0, 8, body, 0)

    def finish(v, carry):
        for n in range(3):
            copy(n, v).wait()
        return carry

    lax.fori_loop(0, 8, finish, 0)


def far_kernel(near, far, cols, turn_far, partial, out, halves, result, sem):
    kc = lax.axis_index("kc")
    set_halves(halves)

    def copy(v):
        row = pl.multiple_of((kc + 2) % 4 * 64, 64)
        at = pl.ds(pl.multiple_of(v * 512, 512), 512)
        return pltpu.make_async_copy(result.at[:, at], out.at[pl.ds(row, 64), at], sem.at[v])

    def body(v, carry):
        for s in range(4):
            u = v * 4 + s
            (turned,) = rotate_points(near, halves, 256 * kc + 8 * u, ((far, turn_far[...]),))
            at = pl.ds(pl.multiple_of(u * LANES, LANES), LANES)
            result[:, at] = dot_t(turned, cols[u]).astype(BF16)
        copy(v).start()
        return carry

    lax.fori_loop(0, 8, body, 0)

    def finish(v, carry):
        copy(v).wait()
        return carry

    lax.fori_loop(0, 8, finish, 0)


def call(kernel, outs, in_specs, out_specs, scratch, flops, aliases=None):
    return pl.pallas_call(
        kernel,
        out_shape=outs,
        in_specs=in_specs,
        out_specs=out_specs,
        scratch_shapes=scratch,
        input_output_aliases=aliases or {},
        compiler_params=pltpu.CompilerParams(vmem_limit_bytes=8 << 20),
        cost_estimate=pl.CostEstimate(flops=flops, bytes_accessed=flops // 10, transcendentals=0),
    )


def shape(*dims):
    return jax.ShapeDtypeStruct(dims, BF16)


def shift(value, by):
    return lax.ppermute(value, "kc", [(i, (i + by) % 4) for i in range(4)])


def partner(value):
    return lax.ppermute(value, "kf_2", [(0, 1), (1, 0)])


def shards(kernel_coarse, coefficients, nearest):
    other = partner(kernel_coarse)
    coef_other = partner(coefficients)
    copies = [pltpu.VMEM((8, 16, 32, LANES), BF16)]
    packed = call(pack_own_kernel, shape(PEERS, 48, LANES), [SMEM, VMEM], VMEM, copies, 1000000)(
        nearest, kernel_coarse
    )
    packed = call(
        pack_other_kernel, shape(PEERS, 48, LANES), [SMEM] + [VMEM] * 4, VMEM, copies, 1000000, {4: 0}
    )(nearest, other, coefficients, coef_other, packed)
    received = lax.all_to_all(packed, ZY, split_axis=0, concat_axis=0, tiled=True)
    block = (PAIRS, LANES)
    up, down, across = call(
        split_kernel, (shape(73, *block), shape(73, *block), shape(9, *block)), [VMEM, VMEM], (VMEM,) * 3, [], 100000
    )(received, coefficients)
    left = shift(up, 1)
    right = shift(down, -1)
    far_coef = shift(across, 2)
    far = jnp.concatenate([shift(left[:PEERS], 1), shift(right[PEERS:64], -1)], axis=0)
    half_masks = pltpu.VMEM((2, *block), BF16)
    partial, cols, turn_far = call(
        middle_kernel,
        (shape(256, 4096), shape(32, LANES, LANES), shape(64, LANES)),
        [SMEM] + [VMEM] * 5,
        (ANY, VMEM, VMEM),
        [
            pltpu.VMEM((4, 8, *block), F32),
            pltpu.VMEM((3, 64, LANES), BF16),
            half_masks,
            pltpu.VMEM((3, 64, 4096), BF16),
            pltpu.SemaphoreType.DMA((3, 8)),
        ],
        8000000,
    )(nearest, received, up, left, right, far_coef)
    return call(
        far_kernel,
        shape(256, 4096),
        [SMEM] + [VMEM] * 3 + [ANY],
        ANY,
        [half_masks, pltpu.VMEM((64, 4096), BF16), pltpu.SemaphoreType.DMA((8,))],
        3000000,
        {4: 0},
    )(nearest, far, cols, turn_far, partial)


def solution(mesh):
    split = Mesh(mesh.devices.reshape(8, 4, 2, mesh.shape["kc"]), KF_KC)
    return jax.shard_map(
        shards,
        mesh=split,
        in_specs=(P(KF, None), P(KF_KC, None), P()),
        out_specs=P(KF, "kc"),
        check_vma=False,
    )
```

```python
import jax
import jax.numpy as jnp
from jax import lax
from jax.experimental import pallas as pl
from jax.experimental.pallas import tpu as pltpu
from jax.sharding import Mesh
from jax.sharding import PartitionSpec as P


KF = ("kf_0", "kf_1", "kf_2")
ZY = ("kf_0", "kf_1")
KF_KC = ("kf_0", "kf_1", "kf_2", "kc")
LANES = 128
PAIRS = 16
POINTS = 4
PEERS = 32
BF16 = jnp.bfloat16
F32 = jnp.float32
VMEM = pl.BlockSpec(memory_space=pltpu.VMEM)
SMEM = pl.BlockSpec(memory_space=pltpu.SMEM)
ANY = pl.BlockSpec(memory_space=pl.ANY)


def iota(shape, dim):
    return lax.broadcasted_iota(jnp.int32, shape, dim)


def dot_t(a, b):
    return lax.dot_general(a, b, (((1,), (1,)), ((), ())), preferred_element_type=F32)


def pack_rows(near, rows, out, copies, at_row):
    kc = lax.axis_index("kc")
    core = lax.axis_index("kf_2")
    for b in range(16):
        block = rows[:, b * LANES : (b + 1) * LANES].astype(F32)
        for s in range(8):
            turned = pltpu.roll(block, s * PAIRS, 1) if s else block
            copies[s, b] = turned.astype(BF16)
    group = iota((PAIRS, LANES), 1) // PAIRS
    base = 16 * core + 4 * kc

    def body(d, carry):
        tile = None
        for j in range(POINTS):
            c = near[32 * d + base + j]
            for lo in range(2):
                at = lo * POINTS + j
                piece = copies[(at - c) & 7, c >> 3, lo * PAIRS : (lo + 1) * PAIRS, :]
                tile = piece if tile is None else jnp.where(group == at, piece, tile)
        out[d, pl.ds(at_row, PAIRS), :] = tile
        return carry

    lax.fori_loop(0, PEERS, body, 0, unroll=4)


def pack_own_kernel(near, own, out, copies):
    pack_rows(near, own, out, copies, pl.multiple_of(lax.axis_index("kf_2") * PAIRS, PAIRS))


def pack_other_kernel(near, other, coef_own, coef_other, half_packed, out, copies):
    core = lax.axis_index("kf_2")
    pack_rows(near, other, out, copies, pl.multiple_of((1 - core) * PAIRS, PAIRS))
    a = coef_own[...].astype(F32)
    o = coef_other[...].astype(F32)
    first = jnp.where(core == 0, a, o)
    second = jnp.where(core == 0, o, a)
    coef = jnp.concatenate(
        [first[:, :LANES], first[:, LANES:], second[:, :LANES], second[:, LANES:]], axis=0
    ).astype(BF16)
    for d in range(PEERS):
        out[d, 2 * PAIRS :, :] = coef


def split_kernel(received, coef_own, up, down, across):
    kc = lax.axis_index("kc")
    mine = coef_own[...].astype(F32)
    mine = jnp.concatenate([mine[:, :LANES], mine[:, LANES:]], axis=0)
    mine = jnp.concatenate([mine, jnp.zeros_like(mine)], axis=0).astype(BF16)
    for zy in range(PEERS):
        for h in range(2):
            block = received[zy, h * PAIRS : (h + 1) * PAIRS, :]
            up[2 * zy + h] = block
            down[2 * zy + h] = block
    for step, target, at in ((1, up, 64), (3, down, 64), (2, across, 0)):
        first = (kc + step) % 4 * 8
        for p in range(8):
            target[at + p] = received[first + p, 2 * PAIRS :, :]
        target[at + 8] = mine


def spread(row_of, count):
    keep = iota((8, LANES), 1) // PAIRS == iota((8, LANES), 0)
    pieces = []
    for p in range(count):
        for half in range(2):
            pieces.append(jnp.where(keep, jnp.broadcast_to(row_of(p, half), (8, LANES)), 0.0))
    return jnp.concatenate(pieces, axis=0).astype(BF16)


def repeat_matrix():
    same = iota((LANES, LANES), 0) % PAIRS == iota((LANES, LANES), 1) % PAIRS
    return jnp.where(same, 1.0, 0.0).astype(BF16)


def set_halves(halves):
    low = iota((PAIRS, LANES), 1) < 64
    halves[0] = jnp.where(low, 1.0, 0.0).astype(BF16)
    halves[1] = jnp.where(low, 0.0, 1.0).astype(BF16)


def pick_points(near, halves, first, sources, picked):
    for i in range(32):
        c = near[first + i]
        keep = halves[c & 1]
        for n, blocks in enumerate(sources):
            picked[n, i * PAIRS : (i + 1) * PAIRS, :] = blocks[c >> 1] * keep


def middle_kernel(
    near, received, mine, left, right, far_coef, out, cols, turn_far, pieces, turns, halves, diag, picked, turned, result, sem
):
    kc = lax.axis_index("kc")
    set_halves(halves)
    repeat = repeat_matrix()
    same = iota((LANES, LANES), 0) // PAIRS == iota((LANES, LANES), 1) // PAIRS
    diag[...] = jnp.where(same, 1.0, 0.0).astype(BF16)
    for p in range(8):
        pieces[kc, p] = received[kc * 8 + p, 2 * PAIRS :, :].astype(F32)
        pieces[(kc + 3) % 4, p] = left[64 + p].astype(F32)
        pieces[(kc + 1) % 4, p] = right[64 + p].astype(F32)
        pieces[(kc + 2) % 4, p] = far_coef[p].astype(F32)
    own_group = iota((64, LANES), 1) // PAIRS % POINTS == iota((64, LANES), 0) // PAIRS
    for n, row in enumerate((mine[72], left[72], right[72], far_coef[8])):
        row = row.astype(F32)
        wide = jnp.dot(
            spread(lambda p, half: row[half * POINTS + p : half * POINTS + p + 1], POINTS),
            repeat,
            preferred_element_type=F32,
        )
        value = jnp.where(own_group, wide, 0.0).astype(BF16)
        if n < 3:
            turns[n] = value
        else:
            turn_far[...] = value

    def copy(n, v):
        row = pl.multiple_of((kc + (0, 3, 1)[n]) % 4 * 64, 64)
        at = pl.ds(v * 1024, 1024)
        return pltpu.make_async_copy(result.at[n, :, at], out.at[pl.ds(row, 64), at], sem.at[n, v])

    def build(v):
        for s in range(4):
            h, par = s // 2, s % 2

            def row_of(p, half):
                r = h * 8 + half * POINTS + p % POINTS
                return pieces[par * 2 + p // POINTS, v, r : r + 1, :]

            wide = jnp.dot(spread(row_of, 8), repeat, preferred_element_type=F32)
            cols[4 * v + s] = wide.astype(BF16) * diag[...]

    def turn(v):
        pick_points(near, halves, 256 * kc + 32 * v, (mine, left, right), picked)
        for n in range(3):
            turned[n * 64 : (n + 1) * 64, v * 512 : (v + 1) * 512] = dot_t(turns[n], picked[n]).astype(BF16)

    def expand(v):
        for u in range(4 * v, 4 * v + 4):
            at = slice(u * LANES, (u + 1) * LANES)
            block = dot_t(turned[:, at], cols[u]).astype(BF16)
            for n in range(3):
                result[n, :, at] = block[n * 64 : (n + 1) * 64]

    for v in range(9):
        if v < 8:
            build(v)
            turn(v)
        if v > 0:
            expand(v - 1)
            if v % 2 == 0:
                for n in range(3):
                    copy(n, v // 2 - 1).start()
    for v in range(4):
        for n in range(3):
            copy(n, v).wait()


def far_kernel(near, far, cols, turn_far, partial, out, halves, picked, turned, result, sem):
    kc = lax.axis_index("kc")
    set_halves(halves)

    def copy(v):
        row = pl.multiple_of((kc + 2) % 4 * 64, 64)
        at = pl.ds(v * 1024, 1024)
        return pltpu.make_async_copy(result.at[:, at], out.at[pl.ds(row, 64), at], sem.at[v])

    for v in range(9):
        if v < 8:
            pick_points(near, halves, 256 * kc + 32 * v, (far,), picked.at[v % 2])
            turned[:, v * 512 : (v + 1) * 512] = dot_t(turn_far[...], picked[v % 2, 0]).astype(BF16)
        if v > 0:
            for u in range(4 * v - 4, 4 * v):
                at = slice(u * LANES, (u + 1) * LANES)
                result[:, at] = dot_t(turned[:, at], cols[u]).astype(BF16)
            if v % 2 == 0:
                copy(v // 2 - 1).start()
    for v in range(4):
        copy(v).wait()


def call(kernel, outs, in_specs, out_specs, scratch, flops, aliases=None):
    return pl.pallas_call(
        kernel,
        out_shape=outs,
        in_specs=in_specs,
        out_specs=out_specs,
        scratch_shapes=scratch,
        input_output_aliases=aliases or {},
        compiler_params=pltpu.CompilerParams(vmem_limit_bytes=8 << 20),
        cost_estimate=pl.CostEstimate(flops=flops, bytes_accessed=flops // 10, transcendentals=0),
    )


def shape(*dims):
    return jax.ShapeDtypeStruct(dims, BF16)


def shift(value, by):
    return lax.ppermute(value, "kc", [(i, (i + by) % 4) for i in range(4)])


def partner(value):
    return lax.ppermute(value, "kf_2", [(0, 1), (1, 0)])


def shards(kernel_coarse, coefficients, nearest):
    other = partner(kernel_coarse)
    coef_other = partner(coefficients)
    copies = [pltpu.VMEM((8, 16, 32, LANES), BF16)]
    packed = call(pack_own_kernel, shape(PEERS, 48, LANES), [SMEM, VMEM], VMEM, copies, 1000000)(
        nearest, kernel_coarse
    )
    packed = call(
        pack_other_kernel, shape(PEERS, 48, LANES), [SMEM] + [VMEM] * 4, VMEM, copies, 1000000, {4: 0}
    )(nearest, other, coefficients, coef_other, packed)
    received = lax.all_to_all(packed, ZY, split_axis=0, concat_axis=0, tiled=True)
    block = (PAIRS, LANES)
    up, down, across = call(
        split_kernel, (shape(73, *block), shape(73, *block), shape(9, *block)), [VMEM, VMEM], (VMEM,) * 3, [], 100000
    )(received, coefficients)
    far_coef = shift(across, 2)
    left = shift(up, 1)
    right = shift(down, -1)
    far = jnp.concatenate([shift(left[:PEERS], 1), shift(right[PEERS:64], -1)], axis=0)
    half_masks = pltpu.VMEM((2, *block), BF16)
    partial, cols, turn_far = call(
        middle_kernel,
        (shape(256, 4096), shape(32, LANES, LANES), shape(64, LANES)),
        [SMEM] + [VMEM] * 5,
        (ANY, VMEM, VMEM),
        [
            pltpu.VMEM((4, 8, *block), F32),
            pltpu.VMEM((3, 64, LANES), BF16),
            half_masks,
            pltpu.VMEM((LANES, LANES), BF16),
            pltpu.VMEM((3, 512, LANES), BF16),
            pltpu.VMEM((192, 4096), BF16),
            pltpu.VMEM((3, 64, 4096), BF16),
            pltpu.SemaphoreType.DMA((3, 4)),
        ],
        8000000,
    )(nearest, received, up, left, right, far_coef)
    return call(
        far_kernel,
        shape(256, 4096),
        [SMEM] + [VMEM] * 3 + [ANY],
        ANY,
        [
            half_masks,
            pltpu.VMEM((2, 1, 512, LANES), BF16),
            pltpu.VMEM((64, 4096), BF16),
            pltpu.VMEM((64, 4096), BF16),
            pltpu.SemaphoreType.DMA((4,)),
        ],
        3000000,
        {4: 0},
    )(nearest, far, cols, turn_far, partial)


def solution(mesh):
    split = Mesh(mesh.devices.reshape(8, 4, 2, mesh.shape["kc"]), KF_KC)
    return jax.shard_map(
        shards,
        mesh=split,
        in_specs=(P(KF, None), P(KF_KC, None), P()),
        out_specs=P(KF, "kc"),
        check_vma=False,
    )
```

```python
import jax
import jax.numpy as jnp
from jax import lax
from jax.experimental import pallas as pl
from jax.experimental.pallas import tpu as pltpu
from jax.sharding import Mesh
from jax.sharding import PartitionSpec as P


KF = ("kf_0", "kf_1", "kf_2")
ZY = ("kf_0", "kf_1")
KF_KC = ("kf_0", "kf_1", "kf_2", "kc")
LANES = 128
PAIRS = 16
POINTS = 4
PEERS = 32
BF16 = jnp.bfloat16
F32 = jnp.float32
VMEM = pl.BlockSpec(memory_space=pltpu.VMEM)
SMEM = pl.BlockSpec(memory_space=pltpu.SMEM)
ANY = pl.BlockSpec(memory_space=pl.ANY)


def iota(shape, dim):
    return lax.broadcasted_iota(jnp.int32, shape, dim)


def dot_t(a, b):
    return lax.dot_general(a, b, (((1,), (1,)), ((), ())), preferred_element_type=F32)


def turn_rows(rows, copies):
    for b in range(16):
        block = rows[:, b * LANES : (b + 1) * LANES].astype(F32)
        for s in range(8):
            turned = pltpu.roll(block, s * PAIRS, 1) if s else block
            copies[s, b] = turned.astype(BF16)


def own_kernel(own, near, coef_own, copies):
    turn_rows(own, copies)


def pack_kernel(near, own_copies, other, coef_own, coef_other, out, other_copies):
    kc = lax.axis_index("kc")
    core = lax.axis_index("kf_2")
    turn_rows(other, other_copies)
    copies = (own_copies, other_copies)
    a = coef_own[...].astype(F32)
    o = coef_other[...].astype(F32)
    first = jnp.where(core == 0, a, o)
    second = jnp.where(core == 0, o, a)
    coef = jnp.concatenate(
        [first[:, :LANES], first[:, LANES:], second[:, :LANES], second[:, LANES:]], axis=0
    ).astype(BF16)
    group = iota((PAIRS, LANES), 1) // PAIRS
    base = 16 * core + 4 * kc

    def body(d, carry):
        tiles = [None, None]
        for j in range(POINTS):
            c = near[32 * d + base + j]
            for lo in range(2):
                at = lo * POINTS + j
                for n in range(2):
                    piece = copies[n][(at - c) & 7, c >> 3, lo * PAIRS : (lo + 1) * PAIRS, :]
                    tiles[n] = piece if tiles[n] is None else jnp.where(group == at, piece, tiles[n])
        out[d, pl.ds(pl.multiple_of(core * PAIRS, PAIRS), PAIRS), :] = tiles[0]
        out[d, pl.ds(pl.multiple_of((1 - core) * PAIRS, PAIRS), PAIRS), :] = tiles[1]
        out[d, 2 * PAIRS :, :] = coef
        return carry

    lax.fori_loop(0, PEERS, body, 0, unroll=4)


def split_kernel(received, coef_own, up_1, up_2, down_1, down_2, across):
    kc = lax.axis_index("kc")
    mine = coef_own[...].astype(F32)
    mine = jnp.concatenate([mine[:, :LANES], mine[:, LANES:]], axis=0)
    mine = jnp.concatenate([mine, jnp.zeros_like(mine)], axis=0).astype(BF16)
    for n in range(64):
        block = received[n // 2, n % 2 * PAIRS : (n % 2 + 1) * PAIRS, :]
        if n < 32:
            up_1[n] = block
            down_2[n] = block
        else:
            up_2[n - 32] = block
            down_1[n - 32] = block
    for step, target, at in ((1, up_2, 32), (3, down_2, 32), (2, across, 0)):
        first = (kc + step) % 4 * 8
        for p in range(8):
            target[at + p] = received[first + p, 2 * PAIRS :, :]
        target[at + 8] = mine


def spread(row_of, count):
    keep = iota((8, LANES), 1) // PAIRS == iota((8, LANES), 0)
    pieces = []
    for p in range(count):
        for half in range(2):
            pieces.append(jnp.where(keep, jnp.broadcast_to(row_of(p, half), (8, LANES)), 0.0))
    return jnp.concatenate(pieces, axis=0).astype(BF16)


def repeat_matrix():
    same = iota((LANES, LANES), 0) % PAIRS == iota((LANES, LANES), 1) % PAIRS
    return jnp.where(same, 1.0, 0.0).astype(BF16)


def set_halves(halves):
    low = iota((PAIRS, LANES), 1) < 64
    halves[0] = jnp.where(low, 1.0, 0.0).astype(BF16)
    halves[1] = jnp.where(low, 0.0, 1.0).astype(BF16)


def pick_points(near, halves, first, sources, picked):
    for i in range(32):
        c = near[first + i]
        keep = halves[c & 1]
        for n, blocks in enumerate(sources):
            if blocks.shape[0] == PEERS:
                block = blocks[c >> 2, pl.ds(pl.multiple_of((c >> 1 & 1) * PAIRS, PAIRS), PAIRS), :]
            else:
                block = blocks[c >> 1]
            picked[n, i * PAIRS : (i + 1) * PAIRS, :] = block * keep


def middle_kernel(
    near, received, coef_own, left, left_coef, right, right_coef, far_coef, out, cols, turn_far,
    pieces, turns, halves, diag, picked, turned, result, sem
):
    kc = lax.axis_index("kc")
    set_halves(halves)
    repeat = repeat_matrix()
    same = iota((LANES, LANES), 0) // PAIRS == iota((LANES, LANES), 1) // PAIRS
    diag[...] = jnp.where(same, 1.0, 0.0).astype(BF16)
    for p in range(8):
        pieces[kc, p] = received[kc * 8 + p, 2 * PAIRS :, :].astype(F32)
        pieces[(kc + 3) % 4, p] = left_coef[32 + p].astype(F32)
        pieces[(kc + 1) % 4, p] = right_coef[32 + p].astype(F32)
        pieces[(kc + 2) % 4, p] = far_coef[p].astype(F32)
    own_group = iota((64, LANES), 1) // PAIRS % POINTS == iota((64, LANES), 0) // PAIRS
    own_rows = coef_own[...].astype(F32)
    rows = [jnp.concatenate([own_rows[:, :LANES], own_rows[:, LANES:]], axis=0)]
    rows += [ref[at].astype(F32) for ref, at in ((left_coef, 40), (right_coef, 40), (far_coef, 8))]
    for n, row in enumerate(rows):
        wide = jnp.dot(
            spread(lambda p, half: row[half * POINTS + p : half * POINTS + p + 1], POINTS),
            repeat,
            preferred_element_type=F32,
        )
        value = jnp.where(own_group, wide, 0.0).astype(BF16)
        if n < 3:
            turns[n] = value
        else:
            turn_far[...] = value

    def copy(n, v):
        row = pl.multiple_of((kc + (0, 3, 1)[n]) % 4 * 64, 64)
        at = pl.ds(v * 1024, 1024)
        return pltpu.make_async_copy(result.at[n, :, at], out.at[pl.ds(row, 64), at], sem.at[n, v])

    def build(v):
        for s in range(4):
            h, par = s // 2, s % 2

            def row_of(p, half):
                r = h * 8 + half * POINTS + p % POINTS
                return pieces[par * 2 + p // POINTS, v, r : r + 1, :]

            wide = jnp.dot(spread(row_of, 8), repeat, preferred_element_type=F32)
            cols[4 * v + s] = wide.astype(BF16) * diag[...]

    def turn(v):
        pick_points(near, halves, 256 * kc + 32 * v, (received, left, right), picked)
        for n in range(3):
            turned[n * 64 : (n + 1) * 64, v * 512 : (v + 1) * 512] = dot_t(turns[n], picked[n]).astype(BF16)

    def expand(v):
        for u in range(4 * v, 4 * v + 4):
            at = slice(u * LANES, (u + 1) * LANES)
            block = dot_t(turned[:, at], cols[u]).astype(BF16)
            for n in range(3):
                result[n, :, at] = block[n * 64 : (n + 1) * 64]

    for v in range(9):
        if v < 8:
            build(v)
            turn(v)
        if v > 0:
            expand(v - 1)
            if v % 2 == 0:
                for n in range(3):
                    copy(n, v // 2 - 1).start()
    for v in range(4):
        for n in range(3):
            copy(n, v).wait()


def far_kernel(near, far, cols, turn_far, partial, out, halves, picked, turned, result, sem):
    kc = lax.axis_index("kc")
    set_halves(halves)

    def copy(v):
        row = pl.multiple_of((kc + 2) % 4 * 64, 64)
        at = pl.ds(v * 1024, 1024)
        return pltpu.make_async_copy(result.at[:, at], out.at[pl.ds(row, 64), at], sem.at[v])

    for v in range(9):
        if v < 8:
            pick_points(near, halves, 256 * kc + 32 * v, (far,), picked.at[v % 2])
            turned[:, v * 512 : (v + 1) * 512] = dot_t(turn_far[...], picked[v % 2, 0]).astype(BF16)
        if v > 0:
            for u in range(4 * v - 4, 4 * v):
                at = slice(u * LANES, (u + 1) * LANES)
                result[:, at] = dot_t(turned[:, at], cols[u]).astype(BF16)
            if v % 2 == 0:
                copy(v // 2 - 1).start()
    for v in range(4):
        copy(v).wait()


def call(kernel, outs, in_specs, out_specs, scratch, flops, aliases=None):
    return pl.pallas_call(
        kernel,
        out_shape=outs,
        in_specs=in_specs,
        out_specs=out_specs,
        scratch_shapes=scratch,
        input_output_aliases=aliases or {},
        compiler_params=pltpu.CompilerParams(vmem_limit_bytes=8 << 20),
        cost_estimate=pl.CostEstimate(flops=flops, bytes_accessed=flops // 10, transcendentals=0),
    )


def shape(*dims):
    return jax.ShapeDtypeStruct(dims, BF16)


def shift(value, by):
    return lax.ppermute(value, "kc", [(i, (i + by) % 4) for i in range(4)])


def partner(value):
    return lax.ppermute(value, "kf_2", [(0, 1), (1, 0)])


def shards(kernel_coarse, coefficients, nearest):
    other = partner(kernel_coarse)
    coef_other = partner(coefficients)
    rotations = (8, 16, 32, LANES)
    own_copies = call(own_kernel, shape(*rotations), [VMEM] * 3, VMEM, [], 1000000)(kernel_coarse, nearest, coefficients)
    packed = call(
        pack_kernel, shape(PEERS, 48, LANES), [SMEM] + [VMEM] * 4, VMEM, [pltpu.VMEM(rotations, BF16)], 1000000
    )(nearest, own_copies, other, coefficients, coef_other)
    received = lax.all_to_all(packed, ZY, split_axis=0, concat_axis=0, tiled=True)
    block = (PAIRS, LANES)
    sizes = (32, 41, 32, 41, 9)
    up_1, up_2, down_1, down_2, across = call(
        split_kernel, tuple(shape(n, *block) for n in sizes), [VMEM, VMEM], (VMEM,) * 5, [], 100000
    )(received, coefficients)
    left_1 = shift(up_1, 1)
    right_1 = shift(down_1, -1)
    far_coef = shift(across, 2)
    left_2 = shift(up_2, 1)
    right_2 = shift(down_2, -1)
    far_1 = shift(left_1, 1)
    far_2 = shift(right_1, -1)
    left = jnp.concatenate([left_1, left_2[:32]], axis=0)
    right = jnp.concatenate([right_2[:32], right_1], axis=0)
    far = jnp.concatenate([far_1, far_2], axis=0)
    half_masks = pltpu.VMEM((2, *block), BF16)
    partial, cols, turn_far = call(
        middle_kernel,
        (shape(256, 4096), shape(32, LANES, LANES), shape(64, LANES)),
        [SMEM] + [VMEM] * 7,
        (ANY, VMEM, VMEM),
        [
            pltpu.VMEM((4, 8, *block), F32),
            pltpu.VMEM((3, 64, LANES), BF16),
            half_masks,
            pltpu.VMEM((LANES, LANES), BF16),
            pltpu.VMEM((3, 512, LANES), BF16),
            pltpu.VMEM((192, 4096), BF16),
            pltpu.VMEM((3, 64, 4096), BF16),
            pltpu.SemaphoreType.DMA((3, 4)),
        ],
        8000000,
    )(nearest, received, coefficients, left, left_2, right, right_2, far_coef)
    return call(
        far_kernel,
        shape(256, 4096),
        [SMEM] + [VMEM] * 3 + [ANY],
        ANY,
        [
            half_masks,
            pltpu.VMEM((2, 1, 512, LANES), BF16),
            pltpu.VMEM((64, 4096), BF16),
            pltpu.VMEM((64, 4096), BF16),
            pltpu.SemaphoreType.DMA((4,)),
        ],
        3000000,
        {4: 0},
    )(nearest, far, cols, turn_far, partial)


def solution(mesh):
    split = Mesh(mesh.devices.reshape(8, 4, 2, mesh.shape["kc"]), KF_KC)
    return jax.shard_map(
        shards,
        mesh=split,
        in_specs=(P(KF, None), P(KF_KC, None), P()),
        out_specs=P(KF, "kc"),
        check_vma=False,
    )
```

```python
import jax
import jax.numpy as jnp
from jax import lax
from jax.experimental import pallas as pl
from jax.experimental.pallas import tpu as pltpu
from jax.sharding import Mesh
from jax.sharding import PartitionSpec as P


KF = ("kf_0", "kf_1", "kf_2")
ZY = ("kf_0", "kf_1")
KF_KC = ("kf_0", "kf_1", "kf_2", "kc")
LANES = 128
PAIRS = 16
POINTS = 4
PEERS = 32
BF16 = jnp.bfloat16
F32 = jnp.float32
VMEM = pl.BlockSpec(memory_space=pltpu.VMEM)
SMEM = pl.BlockSpec(memory_space=pltpu.SMEM)
ANY = pl.BlockSpec(memory_space=pl.ANY)


def iota(shape, dim):
    return lax.broadcasted_iota(jnp.int32, shape, dim)


def dot_t(a, b):
    return lax.dot_general(a, b, (((1,), (1,)), ((), ())), preferred_element_type=F32)


def turn_rows(rows, copies):
    for b in range(16):
        block = rows[:, b * LANES : (b + 1) * LANES].astype(F32)
        for s in range(8):
            turned = pltpu.roll(block, s * PAIRS, 1) if s else block
            copies[s, b] = turned.astype(BF16)


def own_kernel(own, near, coef_own, copies):
    turn_rows(own, copies)


def pack_kernel(near, own_copies, other, coef_own, coef_other, out, other_copies):
    kc = lax.axis_index("kc")
    core = lax.axis_index("kf_2")
    turn_rows(other, other_copies)
    copies = (own_copies, other_copies)
    a = coef_own[...].astype(F32)
    o = coef_other[...].astype(F32)
    first = jnp.where(core == 0, a, o)
    second = jnp.where(core == 0, o, a)
    coef = jnp.concatenate(
        [first[:, :LANES], first[:, LANES:], second[:, :LANES], second[:, LANES:]], axis=0
    ).astype(BF16)
    group = iota((PAIRS, LANES), 1) // PAIRS
    base = 16 * core + 4 * kc

    def body(d, carry):
        tiles = [None, None]
        for j in range(POINTS):
            c = near[32 * d + base + j]
            for lo in range(2):
                at = lo * POINTS + j
                for n in range(2):
                    piece = copies[n][(at - c) & 7, c >> 3, lo * PAIRS : (lo + 1) * PAIRS, :]
                    tiles[n] = piece if tiles[n] is None else jnp.where(group == at, piece, tiles[n])
        out[d, pl.ds(pl.multiple_of(core * PAIRS, PAIRS), PAIRS), :] = tiles[0]
        out[d, pl.ds(pl.multiple_of((1 - core) * PAIRS, PAIRS), PAIRS), :] = tiles[1]
        out[d, 2 * PAIRS :, :] = coef
        return carry

    lax.fori_loop(0, PEERS, body, 0, unroll=4)


def split_kernel(received, coef_own, up_1, up_2, down_1, down_2, across):
    kc = lax.axis_index("kc")
    mine = halves_stacked(coef_own[...].astype(F32))
    mine = jnp.concatenate([mine, jnp.zeros_like(mine)], axis=0).astype(BF16)
    for n in range(64):
        block = received[n // 2, n % 2 * PAIRS : (n % 2 + 1) * PAIRS, :]
        if n < 32:
            up_1[n] = block
            down_2[n] = block
        else:
            up_2[n - 32] = block
            down_1[n - 32] = block
    for step, target, at in ((1, up_1, 32), (3, down_1, 32), (2, across, 0)):
        first = (kc + step) % 4 * 8
        for p in range(8):
            target[at + p] = received[first + p, 2 * PAIRS :, :]
        target[at + 8] = mine


def halves_stacked(coef):
    return jnp.concatenate([coef[:, :LANES], coef[:, LANES:]], axis=0)


def spread(row_of, count):
    keep = iota((8, LANES), 1) // PAIRS == iota((8, LANES), 0)
    pieces = []
    for p in range(count):
        for half in range(2):
            pieces.append(jnp.where(keep, jnp.broadcast_to(row_of(p, half), (8, LANES)), 0.0))
    return jnp.concatenate(pieces, axis=0).astype(BF16)


def repeat_matrix():
    same = iota((LANES, LANES), 0) % PAIRS == iota((LANES, LANES), 1) % PAIRS
    return jnp.where(same, 1.0, 0.0).astype(BF16)


def pair_blocks(low_of, high_of, pairs):
    low = iota((PAIRS, LANES), 1) < 64
    for n in range(64):
        first, second = low_of(n), high_of(n)
        pairs[2 * n] = jnp.where(low, first, pltpu.roll(second.astype(F32), 64, 1).astype(BF16))
        pairs[2 * n + 1] = jnp.where(low, pltpu.roll(first.astype(F32), 64, 1).astype(BF16), second)


def turn_points(near, first, pairs, turn, picked, turned, v):
    for i in range(32):
        picked[v % 2, i * PAIRS : (i + 1) * PAIRS, :] = pairs[near[first + 32 * v + i]]
    turned[:, v * 512 : (v + 1) * 512] = dot_t(turn, picked[v % 2]).astype(BF16)


def expand_points(turned, cols, result, v):
    for u in range(4 * v, 4 * v + 4):
        at = slice(u * LANES, (u + 1) * LANES)
        result[:, at] = jnp.dot(turned[:, at], cols[u], preferred_element_type=F32).astype(BF16)


def middle_kernel(
    near, received, coef_own, left_1, left_2, right_1, far_coef, result, cols, turn_far, pieces, pairs, diag, picked, turned
):
    kc = lax.axis_index("kc")
    repeat = repeat_matrix()
    same = iota((LANES, LANES), 0) // PAIRS == iota((LANES, LANES), 1) // PAIRS
    diag[...] = jnp.where(same, 1.0, 0.0).astype(BF16)

    def turn_of(first, second):
        rows = (first, second)

        def row_of(p, half):
            at = half * POINTS + p % POINTS
            return rows[p // POINTS][at : at + 1]

        return jnp.dot(spread(row_of, 8), repeat, preferred_element_type=F32).astype(BF16) * diag[...]

    turn = turn_of(halves_stacked(coef_own[...].astype(F32)), left_1[40].astype(F32))
    turn_far[...] = turn_of(right_1[40].astype(F32), far_coef[8].astype(F32))
    for p in range(8):
        pieces[kc, p] = received[kc * 8 + p, 2 * PAIRS :, :].astype(F32)
        pieces[(kc + 3) % 4, p] = left_1[32 + p].astype(F32)
        pieces[(kc + 1) % 4, p] = right_1[32 + p].astype(F32)
        pieces[(kc + 2) % 4, p] = far_coef[p].astype(F32)
    pair_blocks(
        lambda n: received[n // 2, n % 2 * PAIRS : (n % 2 + 1) * PAIRS, :],
        lambda n: left_1[n] if n < 32 else left_2[n - 32],
        pairs,
    )

    def build(v):
        for s in range(4):
            h, par = s // 2, s % 2

            def row_of(p, half):
                r = h * 8 + half * POINTS + p % POINTS
                return pieces[par * 2 + p // POINTS, v, r : r + 1, :]

            cols[4 * v + s] = dot_t(repeat, spread(row_of, 8)).astype(BF16) * diag[...]

    for v in range(9):
        if v < 8:
            build(v)
            turn_points(near, 256 * kc, pairs, turn, picked, turned, v)
        if v > 0:
            expand_points(turned, cols, result, v - 1)


def last_kernel(near, right_1, right_2, far_1, far_2, cols, turn_far, first, out, pairs, picked, turned, result, sem):
    kc = lax.axis_index("kc")

    def copy(n, v):
        source = first if n < 2 else result
        row = pl.multiple_of((kc + (0, 3, 1, 2)[n]) % 4 * 64, 64)
        at = pl.ds(v * 1024, 1024)
        return pltpu.make_async_copy(source.at[pl.ds(n % 2 * 64, 64), at], out.at[pl.ds(row, 64), at], sem.at[n, v])

    for v in range(4):
        for n in range(2):
            copy(n, v).start()
    pair_blocks(
        lambda n: right_2[n] if n < 32 else right_1[n - 32], lambda n: far_1[n] if n < 32 else far_2[n - 32], pairs
    )
    turn = turn_far[...]
    for v in range(9):
        if v < 8:
            turn_points(near, 256 * kc, pairs, turn, picked, turned, v)
        if v > 0:
            expand_points(turned, cols, result, v - 1)
            if v % 2 == 0:
                for n in (2, 3):
                    copy(n, v // 2 - 1).start()
    for v in range(4):
        for n in range(4):
            copy(n, v).wait()


def call(kernel, outs, in_specs, out_specs, scratch, flops, aliases=None):
    return pl.pallas_call(
        kernel,
        out_shape=outs,
        in_specs=in_specs,
        out_specs=out_specs,
        scratch_shapes=scratch,
        input_output_aliases=aliases or {},
        compiler_params=pltpu.CompilerParams(vmem_limit_bytes=8 << 20),
        cost_estimate=pl.CostEstimate(flops=flops, bytes_accessed=flops // 10, transcendentals=0),
    )


def shape(*dims):
    return jax.ShapeDtypeStruct(dims, BF16)


def shift(value, by):
    return lax.ppermute(value, "kc", [(i, (i + by) % 4) for i in range(4)])


def partner(value):
    return lax.ppermute(value, "kf_2", [(0, 1), (1, 0)])


def shards(kernel_coarse, coefficients, nearest):
    other = partner(kernel_coarse)
    coef_other = partner(coefficients)
    rotations = (8, 16, 32, LANES)
    own_copies = call(own_kernel, shape(*rotations), [VMEM] * 3, VMEM, [], 1000000)(kernel_coarse.astype(F32), nearest, coefficients)
    packed = call(
        pack_kernel, shape(PEERS, 48, LANES), [SMEM] + [VMEM] * 4, VMEM, [pltpu.VMEM(rotations, BF16)], 1000000
    )(nearest, own_copies, other, coefficients, coef_other)
    received = lax.all_to_all(packed, ZY, split_axis=0, concat_axis=0, tiled=True)
    block = (PAIRS, LANES)
    sizes = (41, 32, 41, 32, 9)
    up_1, up_2, down_1, down_2, across = call(
        split_kernel, tuple(shape(n, *block) for n in sizes), [VMEM, VMEM], (VMEM,) * 5, [], 100000
    )(received, coefficients)
    left_1 = shift(up_1, 1)
    right_1 = shift(down_1, -1)
    far_coef = shift(across, 2)
    left_2 = shift(up_2, 1)
    right_2 = shift(down_2, -1)
    far_1 = shift(left_1[:PEERS], 1)
    far_2 = shift(right_1[:PEERS], -1)
    pairs = pltpu.VMEM((128, *block), BF16)
    picked = pltpu.VMEM((2, 512, LANES), BF16)
    turned = pltpu.VMEM((LANES, 4096), BF16)
    first, cols, turn_far = call(
        middle_kernel,
        (shape(LANES, 4096), shape(32, LANES, LANES), shape(LANES, LANES)),
        [SMEM] + [VMEM] * 6,
        (VMEM,) * 3,
        [pltpu.VMEM((4, 8, *block), F32), pairs, pltpu.VMEM((LANES, LANES), BF16), picked, turned],
        8000000,
    )(nearest, received, coefficients, left_1, left_2, right_1, far_coef)
    return call(
        last_kernel,
        shape(256, 4096),
        [SMEM] + [VMEM] * 7,
        ANY,
        [pairs, picked, turned, turned, pltpu.SemaphoreType.DMA((4, 4))],
        3000000,
    )(nearest, right_1, right_2, far_1, far_2, cols, turn_far, first)


def solution(mesh):
    split = Mesh(mesh.devices.reshape(8, 4, 2, mesh.shape["kc"]), KF_KC)
    return jax.shard_map(
        shards,
        mesh=split,
        in_specs=(P(KF, None), P(KF_KC, None), P()),
        out_specs=P(KF, "kc"),
        check_vma=False,
    )
```

```python
import jax
import jax.numpy as jnp
from jax import lax
from jax.experimental import pallas as pl
from jax.experimental.pallas import tpu as pltpu
from jax.sharding import Mesh
from jax.sharding import PartitionSpec as P


KF = ("kf_0", "kf_1", "kf_2")
ZY = ("kf_0", "kf_1")
KF_KC = ("kf_0", "kf_1", "kf_2", "kc")
LANES = 128
PAIRS = 16
POINTS = 4
PEERS = 32
FINE = 1024
BF16 = jnp.bfloat16
F32 = jnp.float32
VMEM = pl.BlockSpec(memory_space=pltpu.VMEM)
SMEM = pl.BlockSpec(memory_space=pltpu.SMEM)
ANY = pl.BlockSpec(memory_space=pl.ANY)


def iota(shape, dim):
    return lax.broadcasted_iota(jnp.int32, shape, dim)


def dot_t(a, b):
    return lax.dot_general(a, b, (((1,), (1,)), ((), ())), preferred_element_type=F32)


def turn_rows(rows, copies):
    for b in range(16):
        block = rows[:32, b * LANES : (b + 1) * LANES].astype(F32)
        for s in range(8):
            turned = pltpu.roll(block, s * PAIRS, 1) if s else block
            copies[s, b] = turned.astype(BF16)


def own_kernel(fetched, copies, near, coef):
    near[...] = fetched[32:33, :FINE].astype(jnp.int32)
    coef[...] = halves_stacked(fetched[40:44, : 2 * LANES])
    turn_rows(fetched, copies)


def index_copy(near, scalars, sem):
    return pltpu.make_async_copy(near, scalars, sem.at[0])


def pack_kernel(near, own_copies, other, coef_own, coef_other, out, other_copies, scalars, sem):
    fetch = index_copy(near, scalars, sem)
    fetch.start()
    kc = lax.axis_index("kc")
    core = lax.axis_index("kf_2")
    turn_rows(other, other_copies)
    copies = (own_copies, other_copies)
    a = coef_own[...]
    o = halves_stacked(coef_other[...].astype(F32))
    coef = jnp.concatenate([jnp.where(core == 0, a, o), jnp.where(core == 0, o, a)], axis=0).astype(BF16)
    fetch.wait()
    group = iota((PAIRS, LANES), 1) // PAIRS
    base = 16 * core + 4 * kc

    def body(d, carry):
        tiles = [None, None]
        for j in range(POINTS):
            c = scalars[0, 32 * d + base + j]
            for lo in range(2):
                at = lo * POINTS + j
                for n in range(2):
                    piece = copies[n][(at - c) & 7, c >> 3, lo * PAIRS : (lo + 1) * PAIRS, :]
                    tiles[n] = piece if tiles[n] is None else jnp.where(group == at, piece, tiles[n])
        out[d, pl.ds(pl.multiple_of(core * PAIRS, PAIRS), PAIRS), :] = tiles[0]
        out[d, pl.ds(pl.multiple_of((1 - core) * PAIRS, PAIRS), PAIRS), :] = tiles[1]
        out[d, 2 * PAIRS :, :] = coef
        return carry

    lax.fori_loop(0, PEERS, body, 0, unroll=4)


def split_kernel(received, coef_own, up_1, up_2, down_1, down_2, across):
    kc = lax.axis_index("kc")
    mine = coef_own[...]
    mine = jnp.concatenate([mine, jnp.zeros_like(mine)], axis=0).astype(BF16)
    for n in range(64):
        block = received[n // 2, n % 2 * PAIRS : (n % 2 + 1) * PAIRS, :]
        if n < 32:
            up_1[n] = block
            down_2[n] = block
        else:
            up_2[n - 32] = block
            down_1[n - 32] = block
    for step, target, at in ((1, up_1, 32), (3, down_1, 32), (2, across, 0)):
        first = (kc + step) % 4 * 8
        for p in range(8):
            target[at + p] = received[first + p, 2 * PAIRS :, :]
        target[at + 8] = mine


def halves_stacked(coef):
    return jnp.concatenate([coef[:, :LANES], coef[:, LANES:]], axis=0)


def spread(row_of, count):
    keep = iota((8, LANES), 1) // PAIRS == iota((8, LANES), 0)
    pieces = []
    for p in range(count):
        for half in range(2):
            pieces.append(jnp.where(keep, jnp.broadcast_to(row_of(p, half), (8, LANES)), 0.0))
    return jnp.concatenate(pieces, axis=0).astype(BF16)


def repeat_matrix():
    same = iota((LANES, LANES), 0) % PAIRS == iota((LANES, LANES), 1) % PAIRS
    return jnp.where(same, 1.0, 0.0).astype(BF16)


def pair_blocks(low_of, high_of, pairs):
    low = iota((PAIRS, LANES), 1) < 64
    for n in range(64):
        first, second = low_of(n), high_of(n)
        pairs[2 * n] = jnp.where(low, first, pltpu.roll(second.astype(F32), 64, 1).astype(BF16))
        pairs[2 * n + 1] = jnp.where(low, pltpu.roll(first.astype(F32), 64, 1).astype(BF16), second)


def turn_points(scalars, first, pairs, turn, picked, turned, v):
    for i in range(64):
        picked[v % 2, i * PAIRS : (i + 1) * PAIRS, :] = pairs[scalars[0, first + 64 * v + i]]
    turned[:, v * 1024 : (v + 1) * 1024] = dot_t(turn, picked[v % 2]).astype(BF16)


def expand_points(turned, cols, result, v):
    for u in range(8 * v, 8 * v + 8):
        at = slice(u * LANES, (u + 1) * LANES)
        result[:, at] = jnp.dot(turned[:, at], cols[u], preferred_element_type=F32).astype(BF16)


def row_copy(result, out, sem, n, step, v):
    row = pl.multiple_of((lax.axis_index("kc") + step) % 4 * 64, 64)
    at = pl.ds(v * 1024, 1024)
    return pltpu.make_async_copy(result.at[pl.ds(n * 64, 64), at], out.at[pl.ds(row, 64), at], sem.at[1 + 4 * n + v])


def middle_kernel(
    near, received, coef_own, left_1, left_2, right_1, far_coef, out, cols, turn_far,
    pieces, pairs, diag, picked, turned, result, scalars, sem
):
    fetch = index_copy(near, scalars, sem)
    fetch.start()
    kc = lax.axis_index("kc")
    repeat = repeat_matrix()
    same = iota((LANES, LANES), 0) // PAIRS == iota((LANES, LANES), 1) // PAIRS
    diag[...] = jnp.where(same, 1.0, 0.0).astype(BF16)

    def turn_of(first, second):
        rows = (first, second)

        def row_of(p, half):
            at = half * POINTS + p % POINTS
            return rows[p // POINTS][at : at + 1]

        return jnp.dot(spread(row_of, 8), repeat, preferred_element_type=F32).astype(BF16) * diag[...]

    turn = turn_of(coef_own[...], left_1[40].astype(F32))
    turn_far[...] = turn_of(right_1[40].astype(F32), far_coef[8].astype(F32))
    for p in range(8):
        pieces[kc, p] = received[kc * 8 + p, 2 * PAIRS :, :].astype(F32)
        pieces[(kc + 3) % 4, p] = left_1[32 + p].astype(F32)
        pieces[(kc + 1) % 4, p] = right_1[32 + p].astype(F32)
        pieces[(kc + 2) % 4, p] = far_coef[p].astype(F32)
    pair_blocks(
        lambda n: received[n // 2, n % 2 * PAIRS : (n % 2 + 1) * PAIRS, :],
        lambda n: left_1[n] if n < 32 else left_2[n - 32],
        pairs,
    )

    def build(v):
        for s in range(8):
            p_index, h, par = 2 * v + s // 4, s // 2 % 2, s % 2

            def row_of(p, half):
                r = h * 8 + half * POINTS + p % POINTS
                return pieces[par * 2 + p // POINTS, p_index, r : r + 1, :]

            cols[8 * v + s] = dot_t(repeat, spread(row_of, 8)).astype(BF16) * diag[...]

    build(0)
    fetch.wait()
    for v in range(5):
        if v < 4:
            turn_points(scalars, 256 * kc, pairs, turn, picked, turned, v)
            if v > 0:
                build(v)
        if v > 0:
            expand_points(turned, cols, result, v - 1)
            for n, step in enumerate((0, 3)):
                row_copy(result, out, sem, n, step, v - 1).start()
    for v in range(4):
        for n, step in enumerate((0, 3)):
            row_copy(result, out, sem, n, step, v).wait()


def last_kernel(near, right_1, right_2, far_1, far_2, cols, turn_far, partial, out, pairs, picked, turned, result, scalars, sem):
    fetch = index_copy(near, scalars, sem)
    fetch.start()
    kc = lax.axis_index("kc")
    pair_blocks(
        lambda n: right_2[n] if n < 32 else right_1[n - 32], lambda n: far_1[n] if n < 32 else far_2[n - 32], pairs
    )
    turn = turn_far[...]
    fetch.wait()
    for v in range(5):
        if v < 4:
            turn_points(scalars, 256 * kc, pairs, turn, picked, turned, v)
        if v > 0:
            expand_points(turned, cols, result, v - 1)
            for n, step in enumerate((1, 2)):
                row_copy(result, out, sem, n, step, v - 1).start()
    for v in range(4):
        for n, step in enumerate((1, 2)):
            row_copy(result, out, sem, n, step, v).wait()


def call(kernel, outs, in_specs, out_specs, scratch, flops, aliases=None):
    return pl.pallas_call(
        kernel,
        out_shape=outs,
        in_specs=in_specs,
        out_specs=out_specs,
        scratch_shapes=scratch,
        input_output_aliases=aliases or {},
        compiler_params=pltpu.CompilerParams(vmem_limit_bytes=8 << 20),
        cost_estimate=pl.CostEstimate(flops=flops, bytes_accessed=flops // 10, transcendentals=0),
    )


def shape(*dims):
    return jax.ShapeDtypeStruct(dims, BF16)


def shift(value, by):
    return lax.ppermute(value, "kc", [(i, (i + by) % 4) for i in range(4)])


def partner(value):
    return lax.ppermute(value, "kf_2", [(0, 1), (1, 0)])


def shards(kernel_coarse, coefficients, nearest):
    other = partner(kernel_coarse)
    coef_other = partner(coefficients)
    rotations = (8, 16, 32, LANES)
    table = jnp.pad(nearest.reshape(1, FINE), ((32, 15), (0, FINE))).astype(F32)
    rows = jnp.pad(coefficients.astype(F32), ((40, 4), (0, 2 * FINE - 2 * LANES)))
    fetched = jnp.pad(kernel_coarse.astype(F32), ((0, 16), (0, 0))) + table + rows
    scalars = [pltpu.SMEM((1, FINE), jnp.int32), pltpu.SemaphoreType.DMA((9,))]
    own_copies, near, coef_own = call(
        own_kernel,
        (shape(*rotations), jax.ShapeDtypeStruct((1, FINE), jnp.int32), jax.ShapeDtypeStruct((8, LANES), F32)),
        [VMEM],
        (VMEM,) * 3,
        [],
        1000000,
    )(fetched)
    packed = call(
        pack_kernel, shape(PEERS, 48, LANES), [VMEM] * 5, VMEM, [pltpu.VMEM(rotations, BF16)] + scalars, 1000000
    )(near, own_copies, other, coef_own, coef_other)
    received = lax.all_to_all(packed, ZY, split_axis=0, concat_axis=0, tiled=True)
    block = (PAIRS, LANES)
    sizes = (41, 32, 41, 32, 9)
    up_1, up_2, down_1, down_2, across = call(
        split_kernel, tuple(shape(n, *block) for n in sizes), [VMEM, VMEM], (VMEM,) * 5, [], 100000
    )(received, coef_own)
    left_1 = shift(up_1, 1)
    right_1 = shift(down_1, -1)
    far_coef = shift(across, 2)
    left_2 = shift(up_2, 1)
    right_2 = shift(down_2, -1)
    far_1 = shift(left_1[:PEERS], 1)
    far_2 = shift(right_1[:PEERS], -1)
    pairs = pltpu.VMEM((128, *block), BF16)
    picked = pltpu.VMEM((2, 1024, LANES), BF16)
    turned = pltpu.VMEM((LANES, 4096), BF16)
    partial, cols, turn_far = call(
        middle_kernel,
        (shape(256, 4096), shape(32, LANES, LANES), shape(LANES, LANES)),
        [VMEM] * 7,
        (ANY, VMEM, VMEM),
        [pltpu.VMEM((4, 8, *block), F32), pairs, pltpu.VMEM((LANES, LANES), BF16), picked, turned, turned] + scalars,
        8000000,
    )(near, received, coef_own, left_1, left_2, right_1, far_coef)
    return call(
        last_kernel,
        shape(256, 4096),
        [VMEM] * 7 + [ANY],
        ANY,
        [pairs, picked, turned, turned] + scalars,
        3000000,
        {7: 0},
    )(near, right_1, right_2, far_1, far_2, cols, turn_far, partial)


def solution(mesh):
    split = Mesh(mesh.devices.reshape(8, 4, 2, mesh.shape["kc"]), KF_KC)
    return jax.shard_map(
        shards,
        mesh=split,
        in_specs=(P(KF, None), P(KF_KC, None), P()),
        out_specs=P(KF, "kc"),
        check_vma=False,
    )
```

```python
import jax
import jax.numpy as jnp
from jax import lax
from jax.experimental import pallas as pl
from jax.experimental.pallas import tpu as pltpu
from jax.sharding import Mesh
from jax.sharding import PartitionSpec as P


KF = ("kf_0", "kf_1", "kf_2")
ZY = ("kf_0", "kf_1")
KF_KC = ("kf_0", "kf_1", "kf_2", "kc")
LANES = 128
PAIRS = 16
POINTS = 4
PEERS = 32
FINE = 1024
BF16 = jnp.bfloat16
F32 = jnp.float32
VMEM = pl.BlockSpec(memory_space=pltpu.VMEM)
SMEM = pl.BlockSpec(memory_space=pltpu.SMEM)
ANY = pl.BlockSpec(memory_space=pl.ANY)


def iota(shape, dim):
    return lax.broadcasted_iota(jnp.int32, shape, dim)


def dot_t(a, b):
    return lax.dot_general(a, b, (((1,), (1,)), ((), ())), preferred_element_type=F32)


def turn_rows(rows, copies):
    for b in range(16):
        block = rows[:32, b * LANES : (b + 1) * LANES].astype(F32)
        for s in range(8):
            turned = pltpu.roll(block, s * PAIRS, 1) if s else block
            copies[s * 16 + b] = turned.astype(BF16)


def halves_stacked(coef):
    return jnp.concatenate([coef[:, :LANES], coef[:, LANES:]], axis=0)


def own_kernel(fetched, copies, near, slots, coef):
    c = fetched[32:33, :FINE].astype(jnp.int32)
    near[...] = c
    slots[...] = ((iota((1, FINE), 1) % POINTS - c) & 7) * 16 + (c >> 3)
    coef[...] = halves_stacked(fetched[40:44, : 2 * LANES]).astype(BF16)
    turn_rows(fetched, copies)


def index_copy(near, scalars, sem):
    return pltpu.make_async_copy(near, scalars, sem.at[0])


def pack_kernel(slots, own_copies, other, coef, out, other_copies, scalars, sem):
    fetch = index_copy(slots, scalars, sem)
    fetch.start()
    kc = lax.axis_index("kc")
    core = lax.axis_index("kf_2")
    turn_rows(other, other_copies)
    copies = (own_copies, other_copies)
    fetch.wait()
    group = iota((PAIRS, LANES), 1) // PAIRS
    base = 16 * core + 4 * kc

    def body(d, carry):
        tiles = [None, None]
        for j in range(POINTS):
            slot = scalars[0, 32 * d + base + j]
            for lo in range(2):
                for n in range(2):
                    piece = copies[n][slot ^ (64 * lo), lo * PAIRS : (lo + 1) * PAIRS, :]
                    tiles[n] = piece if tiles[n] is None else jnp.where(group == lo * POINTS + j, piece, tiles[n])
        out[d, pl.ds(pl.multiple_of(core * PAIRS, PAIRS), PAIRS), :] = tiles[0]
        out[d, pl.ds(pl.multiple_of((1 - core) * PAIRS, PAIRS), PAIRS), :] = tiles[1]
        out[d, 2 * PAIRS :, :] = coef[...]
        return carry

    lax.fori_loop(0, PEERS, body, 0, unroll=4)


def row_block(received, n):
    return received[n // 2, n % 2 * PAIRS : (n % 2 + 1) * PAIRS, :]


def first_split_kernel(received, coef_own, up_1, coef_half):
    for n in range(48):
        up_1[n] = row_block(received, n)
    mine = coef_own[...].astype(F32)
    up_1[48] = jnp.concatenate([mine, mine], axis=0).astype(BF16)
    for d in range(PEERS):
        coef_half[d] = received[d, 2 * PAIRS :, :]


def second_split_kernel(received, coef_half, coef_other, coef_own, up_2, down_1, down_2, across, home):
    kc = lax.axis_index("kc")
    core = lax.axis_index("kf_2")
    for n in range(16):
        up_2[n] = row_block(received, 48 + n)
        down_2[n] = row_block(received, n)
        down_1[32 + n] = row_block(received, 16 + n)
    for n in range(32):
        down_1[n] = row_block(received, 32 + n)
    for step, target, at in ((0, home, 0), (1, up_2, 16), (3, down_1, 48), (2, across, 0)):
        first = (kc + step) % 4 * 8
        for p in range(8):
            a = coef_half[first + p].astype(F32)
            o = coef_other[first + p].astype(F32)
            both = jnp.concatenate([jnp.where(core == 0, a, o), jnp.where(core == 0, o, a)], axis=0)
            target[at + p] = both.astype(BF16)
    mine = coef_own[...].astype(F32)
    mine = jnp.concatenate([mine, mine], axis=0).astype(BF16)
    down_1[56] = mine
    across[8] = mine


def spread(row_of, count):
    keep = iota((8, LANES), 1) // PAIRS == iota((8, LANES), 0)
    pieces = []
    for p in range(count):
        for half in range(2):
            pieces.append(jnp.where(keep, jnp.broadcast_to(row_of(p, half), (8, LANES)), 0.0))
    return jnp.concatenate(pieces, axis=0).astype(BF16)


def repeat_matrix():
    same = iota((LANES, LANES), 0) % PAIRS == iota((LANES, LANES), 1) % PAIRS
    return jnp.where(same, 1.0, 0.0).astype(BF16)


def pair_blocks(low_of, high_of, pairs):
    low = iota((PAIRS, LANES), 1) < 64
    for n in range(64):
        first, second = low_of(n), high_of(n)
        pairs[2 * n] = jnp.where(low, first, pltpu.roll(second.astype(F32), 64, 1).astype(BF16))
        pairs[2 * n + 1] = jnp.where(low, pltpu.roll(first.astype(F32), 64, 1).astype(BF16), second)


def turn_points(scalars, first, pairs, turn, picked, turned, v):
    for i in range(64):
        picked[v % 2, i * PAIRS : (i + 1) * PAIRS, :] = pairs[scalars[0, first + 64 * v + i]]
    turned[:, v * 1024 : (v + 1) * 1024] = dot_t(turn, picked[v % 2]).astype(BF16)


def expand_points(turned, cols, result, v):
    for u in range(8 * v, 8 * v + 8):
        at = slice(u * LANES, (u + 1) * LANES)
        result[:, at] = jnp.dot(turned[:, at], cols[u], preferred_element_type=F32).astype(BF16)


def row_copy(result, out, sem, n, step, v):
    row = pl.multiple_of((lax.axis_index("kc") + step) % 4 * 64, 64)
    at = pl.ds(v * 1024, 1024)
    return pltpu.make_async_copy(result.at[pl.ds(n * 64, 64), at], out.at[pl.ds(row, 64), at], sem.at[1 + 4 * n + v])


def middle_kernel(
    near, received, coef_own, home, left_1, left_2, right_1, far_coef, out, cols, turn_far,
    pieces, pairs, diag, picked, turned, result, scalars, sem
):
    fetch = index_copy(near, scalars, sem)
    fetch.start()
    kc = lax.axis_index("kc")
    repeat = repeat_matrix()
    same = iota((LANES, LANES), 0) // PAIRS == iota((LANES, LANES), 1) // PAIRS
    diag[...] = jnp.where(same, 1.0, 0.0).astype(BF16)

    def turn_of(first, second):
        rows = (first, second)

        def row_of(p, half):
            at = half * POINTS + p % POINTS
            return rows[p // POINTS][at : at + 1]

        return jnp.dot(spread(row_of, 8), repeat, preferred_element_type=F32).astype(BF16) * diag[...]

    turn = turn_of(coef_own[...].astype(F32), left_1[48].astype(F32))
    turn_far[...] = turn_of(right_1[56].astype(F32), far_coef[8].astype(F32))
    for p in range(8):
        pieces[kc, p] = home[p].astype(F32)
        pieces[(kc + 3) % 4, p] = left_2[16 + p].astype(F32)
        pieces[(kc + 1) % 4, p] = right_1[48 + p].astype(F32)
        pieces[(kc + 2) % 4, p] = far_coef[p].astype(F32)
    pair_blocks(
        lambda n: row_block(received, n), lambda n: left_1[n] if n < 48 else left_2[n - 48], pairs
    )

    def build(v):
        for s in range(8):
            p_index, h, par = 2 * v + s // 4, s // 2 % 2, s % 2

            def row_of(p, half):
                r = h * 8 + half * POINTS + p % POINTS
                return pieces[par * 2 + p // POINTS, p_index, r : r + 1, :]

            cols[8 * v + s] = dot_t(repeat, spread(row_of, 8)).astype(BF16) * diag[...]

    build(0)
    fetch.wait()
    for v in range(5):
        if v < 4:
            turn_points(scalars, 256 * kc, pairs, turn, picked, turned, v)
            if v > 0:
                build(v)
        if v > 0:
            expand_points(turned, cols, result, v - 1)
            for n, step in enumerate((0, 3)):
                row_copy(result, out, sem, n, step, v - 1).start()
    for v in range(4):
        for n, step in enumerate((0, 3)):
            row_copy(result, out, sem, n, step, v).wait()


def last_kernel(near, right_1, right_2, far_1, far_2, cols, turn_far, partial, out, pairs, picked, turned, result, scalars, sem):
    fetch = index_copy(near, scalars, sem)
    fetch.start()
    kc = lax.axis_index("kc")
    pair_blocks(
        lambda n: right_2[n] if n < 16 else right_1[n + 16 if n < 32 else n - 32], lambda n: far_1[n] if n < 32 else far_2[n - 32], pairs
    )
    turn = turn_far[...]
    fetch.wait()
    for v in range(5):
        if v < 4:
            turn_points(scalars, 256 * kc, pairs, turn, picked, turned, v)
        if v > 0:
            expand_points(turned, cols, result, v - 1)
            for n, step in enumerate((1, 2)):
                row_copy(result, out, sem, n, step, v - 1).start()
    for v in range(4):
        for n, step in enumerate((1, 2)):
            row_copy(result, out, sem, n, step, v).wait()


def call(kernel, outs, in_specs, out_specs, scratch, flops, aliases=None):
    return pl.pallas_call(
        kernel,
        out_shape=outs,
        in_specs=in_specs,
        out_specs=out_specs,
        scratch_shapes=scratch,
        input_output_aliases=aliases or {},
        compiler_params=pltpu.CompilerParams(vmem_limit_bytes=8 << 20),
        cost_estimate=pl.CostEstimate(flops=flops, bytes_accessed=flops // 10, transcendentals=0),
    )


def shape(*dims):
    return jax.ShapeDtypeStruct(dims, BF16)


def shift(value, by):
    return lax.ppermute(value, "kc", [(i, (i + by) % 4) for i in range(4)])


def partner(value):
    return lax.ppermute(value, "kf_2", [(0, 1), (1, 0)])


def shards(kernel_coarse, coefficients, nearest):
    other = partner(kernel_coarse)
    rotations = (128, 32, LANES)
    block = (PAIRS, LANES)
    table = jnp.pad(nearest.reshape(1, FINE), ((32, 15), (0, FINE))).astype(F32)
    rows = jnp.pad(coefficients.astype(F32), ((40, 4), (0, 2 * FINE - 2 * LANES)))
    fetched = jnp.pad(kernel_coarse.astype(F32), ((0, 16), (0, 0))) + table + rows
    scalars = [pltpu.SMEM((1, FINE), jnp.int32), pltpu.SemaphoreType.DMA((9,))]
    index = jax.ShapeDtypeStruct((1, FINE), jnp.int32)
    own_copies, near, slots, coef_own = call(
        own_kernel, (shape(*rotations), index, index, shape(8, LANES)), [VMEM], (VMEM,) * 4, [], 1000000
    )(fetched)
    packed = call(
        pack_kernel, shape(PEERS, 40, LANES), [VMEM] * 4, VMEM, [pltpu.VMEM(rotations, BF16)] + scalars, 1000000
    )(slots, own_copies, other, coef_own)
    received = lax.all_to_all(packed, ZY, split_axis=0, concat_axis=0, tiled=True)
    up_1, coef_half = call(
        first_split_kernel, (shape(49, *block), shape(PEERS, 8, LANES)), [VMEM] * 2, (VMEM,) * 2, [], 100000
    )(received, coef_own)
    coef_other = partner(coef_half)
    left_1 = shift(up_1, 1)
    sizes = (24, 57, 16, 9, 8)
    up_2, down_1, down_2, across, home = call(
        second_split_kernel, tuple(shape(n, *block) for n in sizes), [VMEM] * 4, (VMEM,) * 5, [], 100000
    )(received, coef_half, coef_other, coef_own)
    right_1 = shift(down_1, -1)
    far_coef = shift(across, 2)
    left_2 = shift(up_2, 1)
    right_2 = shift(down_2, -1)
    far_1 = shift(left_1[:PEERS], 1)
    far_2 = shift(right_1[:PEERS], -1)
    pairs = pltpu.VMEM((128, *block), BF16)
    picked = pltpu.VMEM((2, 1024, LANES), BF16)
    turned = pltpu.VMEM((LANES, 4096), BF16)
    partial, cols, turn_far = call(
        middle_kernel,
        (shape(256, 4096), shape(32, LANES, LANES), shape(LANES, LANES)),
        [VMEM] * 8,
        (ANY, VMEM, VMEM),
        [pltpu.VMEM((4, 8, *block), F32), pairs, pltpu.VMEM((LANES, LANES), BF16), picked, turned, turned] + scalars,
        8000000,
    )(near, received, coef_own, home, left_1, left_2, right_1, far_coef)
    return call(
        last_kernel,
        shape(256, 4096),
        [VMEM] * 7 + [ANY],
        ANY,
        [pairs, picked, turned, turned] + scalars,
        3000000,
        {7: 0},
    )(near, right_1, right_2, far_1, far_2, cols, turn_far, partial)


def solution(mesh):
    split = Mesh(mesh.devices.reshape(8, 4, 2, mesh.shape["kc"]), KF_KC)
    return jax.shard_map(
        shards,
        mesh=split,
        in_specs=(P(KF, None), P(KF_KC, None), P()),
        out_specs=P(KF, "kc"),
        check_vma=False,
    )
```

```python
import jax
import jax.numpy as jnp
from jax import lax
from jax.experimental import pallas as pl
from jax.experimental.pallas import tpu as pltpu
from jax.sharding import Mesh
from jax.sharding import PartitionSpec as P


KF = ("kf_0", "kf_1", "kf_2")
ZY = ("kf_0", "kf_1")
KF_KC = ("kf_0", "kf_1", "kf_2", "kc")
LANES = 128
PAIRS = 16
POINTS = 4
PEERS = 32
FINE = 1024
BF16 = jnp.bfloat16
F32 = jnp.float32
VMEM = pl.BlockSpec(memory_space=pltpu.VMEM)
SMEM = pl.BlockSpec(memory_space=pltpu.SMEM)
ANY = pl.BlockSpec(memory_space=pl.ANY)


def iota(shape, dim):
    return lax.broadcasted_iota(jnp.int32, shape, dim)


def dot_t(a, b):
    return lax.dot_general(a, b, (((1,), (1,)), ((), ())), preferred_element_type=F32)


def turn_rows(rows, copies):
    for b in range(16):
        block = rows[:32, b * LANES : (b + 1) * LANES].astype(F32)
        for s in range(8):
            turned = pltpu.roll(block, s * PAIRS, 1) if s else block
            copies[s * 16 + b] = turned.astype(BF16)


def halves_stacked(coef):
    return jnp.concatenate([coef[:, :LANES], coef[:, LANES:]], axis=0)


def own_kernel(fetched, copies, near, slots, coef):
    c = fetched[32:33, :FINE].astype(jnp.int32)
    near[...] = c
    slots[...] = ((iota((1, FINE), 1) % POINTS - c) & 7) * 16 + (c >> 3)
    coef[...] = halves_stacked(fetched[40:44, : 2 * LANES]).astype(BF16)
    turn_rows(fetched, copies)


def index_copy(near, scalars, sem):
    return pltpu.make_async_copy(near, scalars, sem.at[0])


def pack_kernel(slots, own_copies, other, coef, out, other_copies, scalars, sem):
    fetch = index_copy(slots, scalars, sem)
    fetch.start()
    kc = lax.axis_index("kc")
    core = lax.axis_index("kf_2")
    turn_rows(other, other_copies)
    copies = (own_copies, other_copies)
    fetch.wait()
    group = iota((PAIRS, LANES), 1) // PAIRS
    base = 16 * core + 4 * kc

    def body(d, carry):
        tiles = [None, None]
        for j in range(POINTS):
            slot = scalars[0, 32 * d + base + j]
            for lo in range(2):
                for n in range(2):
                    piece = copies[n][slot ^ (64 * lo), lo * PAIRS : (lo + 1) * PAIRS, :]
                    tiles[n] = piece if tiles[n] is None else jnp.where(group == lo * POINTS + j, piece, tiles[n])
        out[d, pl.ds(pl.multiple_of(core * PAIRS, PAIRS), PAIRS), :] = tiles[0]
        out[d, pl.ds(pl.multiple_of((1 - core) * PAIRS, PAIRS), PAIRS), :] = tiles[1]
        out[d, 2 * PAIRS :, :] = coef[...]
        return carry

    lax.fori_loop(0, PEERS, body, 0, unroll=4)


def row_block(received, n):
    return received[n // 2, n % 2 * PAIRS : (n % 2 + 1) * PAIRS, :]


def row_coefficients(coef_own):
    mine = coef_own[...].astype(F32)
    return jnp.concatenate([mine, mine], axis=0).astype(BF16)


def put_pieces(received, kc, target, at):
    for p in range(8):
        target[at + p // 2, p % 2 * 8 : p % 2 * 8 + 8, :] = received[kc * 8 + p, 2 * PAIRS :, :]


def split_kernel(received, coef_own, up_1, up_2, down_1, down_2, across):
    kc = lax.axis_index("kc")
    mine = row_coefficients(coef_own)
    for n in range(32):
        up_1[n] = row_block(received, n)
        down_2[n] = row_block(received, n)
        up_2[n] = row_block(received, 32 + n)
        down_1[n] = row_block(received, 32 + n)
    for step, target, at in ((1, up_1, 32), (3, down_1, 32), (2, across, 0)):
        put_pieces(received, (kc + step) % 4, target, at)
        target[at + 4] = mine


def collect_kernel(received, left_1, right_1, far_coef, collected):
    put_pieces(received, lax.axis_index("kc"), collected, 0)
    for n in range(4):
        collected[4 + n] = left_1[32 + n]
        collected[8 + n] = right_1[32 + n]
        collected[12 + n] = far_coef[n]


def spread(row_of, count):
    keep = iota((8, LANES), 1) // PAIRS == iota((8, LANES), 0)
    pieces = []
    for p in range(count):
        for half in range(2):
            pieces.append(jnp.where(keep, jnp.broadcast_to(row_of(p, half), (8, LANES)), 0.0))
    return jnp.concatenate(pieces, axis=0).astype(BF16)


def repeat_matrix():
    same = iota((LANES, LANES), 0) % PAIRS == iota((LANES, LANES), 1) % PAIRS
    return jnp.where(same, 1.0, 0.0).astype(BF16)


def pair_blocks(low_of, high_of, pairs):
    low = iota((PAIRS, LANES), 1) < 64
    for n in range(64):
        first, second = low_of(n), high_of(n)
        pairs[2 * n] = jnp.where(low, first, pltpu.roll(second.astype(F32), 64, 1).astype(BF16))
        pairs[2 * n + 1] = jnp.where(low, pltpu.roll(first.astype(F32), 64, 1).astype(BF16), second)


def turn_points(scalars, first, pairs, turn, picked, turned, v):
    for i in range(64):
        picked[v % 2, i * PAIRS : (i + 1) * PAIRS, :] = pairs[scalars[0, first + 64 * v + i]]
    turned[:, v * 1024 : (v + 1) * 1024] = dot_t(turn, picked[v % 2]).astype(BF16)


def expand_points(turned, cols, result, v):
    for u in range(8 * v, 8 * v + 8):
        at = slice(u * LANES, (u + 1) * LANES)
        result[:, at] = jnp.dot(turned[:, at], cols[u], preferred_element_type=F32).astype(BF16)


def row_copy(result, out, sem, n, step, v):
    row = pl.multiple_of((lax.axis_index("kc") + step) % 4 * 64, 64)
    at = pl.ds(v * 1024, 1024)
    return pltpu.make_async_copy(result.at[pl.ds(n * 64, 64), at], out.at[pl.ds(row, 64), at], sem.at[1 + 4 * n + v])


def middle_kernel(
    near, received, coef_own, coef_half, coef_other, left_1, left_2, right_1, far_coef, out, cols, turn_far,
    pieces, pairs, diag, picked, turned, result, scalars, sem
):
    fetch = index_copy(near, scalars, sem)
    fetch.start()
    kc = lax.axis_index("kc")
    repeat = repeat_matrix()
    same = iota((LANES, LANES), 0) // PAIRS == iota((LANES, LANES), 1) // PAIRS
    diag[...] = jnp.where(same, 1.0, 0.0).astype(BF16)

    def turn_of(first, second):
        rows = (first, second)

        def row_of(p, half):
            at = half * POINTS + p % POINTS
            return rows[p // POINTS][at : at + 1]

        return jnp.dot(spread(row_of, 8), repeat, preferred_element_type=F32).astype(BF16) * diag[...]

    turn = turn_of(coef_own[...].astype(F32), left_1[36].astype(F32))
    turn_far[...] = turn_of(right_1[36].astype(F32), far_coef[4].astype(F32))
    core = lax.axis_index("kf_2")
    for n, step in enumerate((0, 3, 1, 2)):
        for p in range(8):
            for owner, source in ((core, coef_half), (1 - core, coef_other)):
                piece = source[4 * n + p // 2, p % 2 * 8 : p % 2 * 8 + 8, :].astype(F32)
                pieces[(kc + step) % 4, p, pl.ds(pl.multiple_of(owner * 8, 8), 8), :] = piece
    pair_blocks(
        lambda n: row_block(received, n), lambda n: left_1[n] if n < 32 else left_2[n - 32], pairs
    )

    def build(v):
        for s in range(8):
            p_index, h, par = 2 * v + s // 4, s // 2 % 2, s % 2

            def row_of(p, half):
                r = h * 8 + half * POINTS + p % POINTS
                return pieces[par * 2 + p // POINTS, p_index, r : r + 1, :]

            cols[8 * v + s] = dot_t(repeat, spread(row_of, 8)).astype(BF16) * diag[...]

    build(0)
    fetch.wait()
    for v in range(5):
        if v < 4:
            turn_points(scalars, 256 * kc, pairs, turn, picked, turned, v)
            if v > 0:
                build(v)
        if v > 0:
            expand_points(turned, cols, result, v - 1)
            for n, step in enumerate((0, 3)):
                row_copy(result, out, sem, n, step, v - 1).start()
    for v in range(4):
        for n, step in enumerate((0, 3)):
            row_copy(result, out, sem, n, step, v).wait()


def last_kernel(near, right_1, right_2, far_1, far_2, cols, turn_far, partial, out, pairs, picked, turned, result, scalars, sem):
    fetch = index_copy(near, scalars, sem)
    fetch.start()
    kc = lax.axis_index("kc")
    pair_blocks(
        lambda n: right_2[n] if n < 32 else right_1[n - 32], lambda n: far_1[n] if n < 32 else far_2[n - 32], pairs
    )
    turn = turn_far[...]
    fetch.wait()
    for v in range(5):
        if v < 4:
            turn_points(scalars, 256 * kc, pairs, turn, picked, turned, v)
        if v > 0:
            expand_points(turned, cols, result, v - 1)
            for n, step in enumerate((1, 2)):
                row_copy(result, out, sem, n, step, v - 1).start()
    for v in range(4):
        for n, step in enumerate((1, 2)):
            row_copy(result, out, sem, n, step, v).wait()


def call(kernel, outs, in_specs, out_specs, scratch, flops, aliases=None):
    return pl.pallas_call(
        kernel,
        out_shape=outs,
        in_specs=in_specs,
        out_specs=out_specs,
        scratch_shapes=scratch,
        input_output_aliases=aliases or {},
        compiler_params=pltpu.CompilerParams(vmem_limit_bytes=8 << 20),
        cost_estimate=pl.CostEstimate(flops=flops, bytes_accessed=flops // 10, transcendentals=0),
    )


def shape(*dims):
    return jax.ShapeDtypeStruct(dims, BF16)


def shift(value, by):
    return lax.ppermute(value, "kc", [(i, (i + by) % 4) for i in range(4)])


def partner(value):
    return lax.ppermute(value, "kf_2", [(0, 1), (1, 0)])


def shards(kernel_coarse, coefficients, nearest):
    other = partner(kernel_coarse)
    rotations = (128, 32, LANES)
    block = (PAIRS, LANES)
    table = jnp.pad(nearest.reshape(1, FINE), ((32, 15), (0, FINE))).astype(F32)
    rows = jnp.pad(coefficients.astype(F32), ((40, 4), (0, 2 * FINE - 2 * LANES)))
    fetched = jnp.pad(kernel_coarse.astype(F32), ((0, 16), (0, 0))) + table + rows
    scalars = [pltpu.SMEM((1, FINE), jnp.int32), pltpu.SemaphoreType.DMA((9,))]
    index = jax.ShapeDtypeStruct((1, FINE), jnp.int32)
    own_copies, near, slots, coef_own = call(
        own_kernel, (shape(*rotations), index, index, shape(8, LANES)), [VMEM], (VMEM,) * 4, [], 1000000
    )(fetched)
    packed = call(
        pack_kernel, shape(PEERS, 40, LANES), [VMEM] * 4, VMEM, [pltpu.VMEM(rotations, BF16)] + scalars, 1000000
    )(slots, own_copies, other, coef_own)
    received = lax.all_to_all(packed, ZY, split_axis=0, concat_axis=0, tiled=True)
    sizes = (37, 32, 37, 32, 5)
    up_1, up_2, down_1, down_2, across = call(
        split_kernel, tuple(shape(n, *block) for n in sizes), [VMEM] * 2, (VMEM,) * 5, [], 100000
    )(received, coef_own)
    left_1 = shift(up_1, 1)
    right_1 = shift(down_1, -1)
    far_coef = shift(across, 2)
    left_2 = shift(up_2, 1)
    right_2 = shift(down_2, -1)
    far_1 = shift(left_1[:PEERS], 1)
    far_2 = shift(right_1[:PEERS], -1)
    coef_half = call(collect_kernel, shape(16, *block), [VMEM] * 4, VMEM, [], 100000)(received, left_1, right_1, far_coef)
    coef_other = partner(coef_half)
    pairs = pltpu.VMEM((128, *block), BF16)
    picked = pltpu.VMEM((2, 1024, LANES), BF16)
    turned = pltpu.VMEM((LANES, 4096), BF16)
    partial, cols, turn_far = call(
        middle_kernel,
        (shape(256, 4096), shape(32, LANES, LANES), shape(LANES, LANES)),
        [VMEM] * 9,
        (ANY, VMEM, VMEM),
        [pltpu.VMEM((4, 8, *block), F32), pairs, pltpu.VMEM((LANES, LANES), BF16), picked, turned, turned] + scalars,
        8000000,
    )(near, received, coef_own, coef_half, coef_other, left_1, left_2, right_1, far_coef)
    return call(
        last_kernel,
        shape(256, 4096),
        [VMEM] * 7 + [ANY],
        ANY,
        [pairs, picked, turned, turned] + scalars,
        3000000,
        {7: 0},
    )(near, right_1, right_2, far_1, far_2, cols, turn_far, partial)


def solution(mesh):
    split = Mesh(mesh.devices.reshape(8, 4, 2, mesh.shape["kc"]), KF_KC)
    return jax.shard_map(
        shards,
        mesh=split,
        in_specs=(P(KF, None), P(KF_KC, None), P()),
        out_specs=P(KF, "kc"),
        check_vma=False,
    )
```

```python
import jax
import jax.numpy as jnp
from jax import lax
from jax.experimental import pallas as pl
from jax.experimental.pallas import tpu as pltpu
from jax.sharding import Mesh
from jax.sharding import PartitionSpec as P


KF = ("kf_0", "kf_1", "kf_2")
ZY = ("kf_0", "kf_1")
KF_KC = ("kf_0", "kf_1", "kf_2", "kc")
LANES = 128
PAIRS = 16
POINTS = 4
PEERS = 32
FINE = 1024
BF16 = jnp.bfloat16
F32 = jnp.float32
VMEM = pl.BlockSpec(memory_space=pltpu.VMEM)
SMEM = pl.BlockSpec(memory_space=pltpu.SMEM)
ANY = pl.BlockSpec(memory_space=pl.ANY)


def iota(shape, dim):
    return lax.broadcasted_iota(jnp.int32, shape, dim)


def dot_t(a, b):
    return lax.dot_general(a, b, (((1,), (1,)), ((), ())), preferred_element_type=F32)


def turn_rows(rows, copies):
    for b in range(16):
        block = rows[:32, b * LANES : (b + 1) * LANES].astype(F32)
        for s in range(8):
            turned = pltpu.roll(block, s * PAIRS, 1) if s else block
            copies[s * 16 + b] = turned.astype(BF16)


def halves_stacked(coef):
    return jnp.concatenate([coef[:, :LANES], coef[:, LANES:]], axis=0)


def own_kernel(fetched, copies, near, slots, coef):
    c = fetched[32:33, :FINE].astype(jnp.int32)
    near[...] = c
    slots[...] = ((iota((1, FINE), 1) % POINTS - c) & 7) * 16 + (c >> 3)
    coef[...] = halves_stacked(fetched[40:44, : 2 * LANES]).astype(BF16)
    turn_rows(fetched, copies)


def index_copy(near, scalars, sem):
    return pltpu.make_async_copy(near, scalars, sem.at[0])


def pack_kernel(slots, own_copies, other, coef, out, other_copies, scalars, sem):
    fetch = index_copy(slots, scalars, sem)
    fetch.start()
    kc = lax.axis_index("kc")
    core = lax.axis_index("kf_2")
    turn_rows(other, other_copies)
    copies = (own_copies, other_copies)
    fetch.wait()
    group = iota((PAIRS, LANES), 1) // PAIRS
    base = 16 * core + 4 * kc

    def body(d, carry):
        tiles = [None, None]
        for j in range(POINTS):
            slot = scalars[0, 32 * d + base + j]
            for lo in range(2):
                for n in range(2):
                    piece = copies[n][slot ^ (64 * lo), lo * PAIRS : (lo + 1) * PAIRS, :]
                    tiles[n] = piece if tiles[n] is None else jnp.where(group == lo * POINTS + j, piece, tiles[n])
        out[d, pl.ds(pl.multiple_of(core * PAIRS, PAIRS), PAIRS), :] = tiles[0]
        out[d, pl.ds(pl.multiple_of((1 - core) * PAIRS, PAIRS), PAIRS), :] = tiles[1]
        out[d, 2 * PAIRS :, :] = coef[...]
        return carry

    lax.fori_loop(0, PEERS, body, 0, unroll=4)


def row_block(received, n):
    return received[n // 2, n % 2 * PAIRS : (n % 2 + 1) * PAIRS, :]


def row_coefficients(coef_own):
    mine = coef_own[...].astype(F32)
    return jnp.concatenate([mine, mine], axis=0).astype(BF16)


def put_pieces(received, kc, target, at):
    for p in range(8):
        target[at + p // 2, p % 2 * 8 : p % 2 * 8 + 8, :] = received[kc * 8 + p, 2 * PAIRS :, :]


def split_kernel(received, coef_own, mine, up, down, across):
    kc = lax.axis_index("kc")
    for n in range(64):
        block = row_block(received, n)
        for target in (mine, up, down):
            target[n] = block
    for step, target, at in ((1, up, 64), (3, down, 64), (2, across, 0)):
        put_pieces(received, (kc + step) % 4, target, at)
        target[at + 4] = row_coefficients(coef_own)


def collect_kernel(received, left, right, far_coef, collected):
    put_pieces(received, lax.axis_index("kc"), collected, 0)
    for n in range(4):
        collected[4 + n] = left[64 + n]
        collected[8 + n] = right[64 + n]
        collected[12 + n] = far_coef[n]


def spread(row_of, count):
    keep = iota((8, LANES), 1) // PAIRS == iota((8, LANES), 0)
    pieces = []
    for p in range(count):
        for half in range(2):
            pieces.append(jnp.where(keep, jnp.broadcast_to(row_of(p, half), (8, LANES)), 0.0))
    return jnp.concatenate(pieces, axis=0).astype(BF16)


def repeat_matrix():
    same = iota((LANES, LANES), 0) % PAIRS == iota((LANES, LANES), 1) % PAIRS
    return jnp.where(same, 1.0, 0.0).astype(BF16)


def pair_blocks(low_of, high_of, pairs):
    low = iota((PAIRS, LANES), 1) < 64
    for n in range(64):
        first, second = low_of(n), high_of(n)
        pairs[2 * n] = jnp.where(low, first, pltpu.roll(second.astype(F32), 64, 1).astype(BF16))
        pairs[2 * n + 1] = jnp.where(low, pltpu.roll(first.astype(F32), 64, 1).astype(BF16), second)


def turn_points(scalars, first, pairs, turn, picked, turned, v):
    for i in range(64):
        picked[v % 2, i * PAIRS : (i + 1) * PAIRS, :] = pairs[scalars[0, first + 64 * v + i]]
    turned[:, v * 1024 : (v + 1) * 1024] = dot_t(turn, picked[v % 2]).astype(BF16)


def expand_points(turned, cols, result, v):
    for u in range(8 * v, 8 * v + 8):
        at = slice(u * LANES, (u + 1) * LANES)
        result[:, at] = jnp.dot(turned[:, at], cols[u], preferred_element_type=F32).astype(BF16)


def row_copy(result, out, sem, n, step, v):
    row = pl.multiple_of((lax.axis_index("kc") + step) % 4 * 64, 64)
    at = pl.ds(v * 1024, 1024)
    return pltpu.make_async_copy(result.at[pl.ds(n * 64, 64), at], out.at[pl.ds(row, 64), at], sem.at[1 + 4 * n + v])


def diagonal():
    same = iota((LANES, LANES), 0) // PAIRS == iota((LANES, LANES), 1) // PAIRS
    return jnp.where(same, 1.0, 0.0).astype(BF16)


def turn_of(first, second, repeat, diag):
    rows = (first.astype(F32), second.astype(F32))

    def row_of(p, half):
        at = half * POINTS + p % POINTS
        return rows[p // POINTS][at : at + 1]

    return jnp.dot(spread(row_of, 8), repeat, preferred_element_type=F32).astype(BF16) * diag


def turn_kernel(near, mine, coef_own, left, turned, pairs, picked, scalars, sem):
    fetch = index_copy(near, scalars, sem)
    fetch.start()
    kc = lax.axis_index("kc")
    turn = turn_of(coef_own[...], left[68], repeat_matrix(), diagonal())
    pair_blocks(lambda n: mine[n], lambda n: left[n], pairs)
    fetch.wait()
    for v in range(4):
        turn_points(scalars, 256 * kc, pairs, turn, picked, turned, v)


def middle_kernel(
    coef_half, coef_other, right, far_coef, turned, out, cols, turn_far, pieces, diag, result, sem
):
    kc = lax.axis_index("kc")
    repeat = repeat_matrix()
    diag[...] = diagonal()
    turn_far[...] = turn_of(right[68], far_coef[4], repeat, diag[...])
    core = lax.axis_index("kf_2")
    for n, step in enumerate((0, 3, 1, 2)):
        for p in range(8):
            for owner, source in ((core, coef_half), (1 - core, coef_other)):
                piece = source[4 * n + p // 2, p % 2 * 8 : p % 2 * 8 + 8, :].astype(F32)
                pieces[(kc + step) % 4, p, pl.ds(pl.multiple_of(owner * 8, 8), 8), :] = piece

    def build(v):
        for s in range(8):
            p_index, h, par = 2 * v + s // 4, s // 2 % 2, s % 2

            def row_of(p, half):
                r = h * 8 + half * POINTS + p % POINTS
                return pieces[par * 2 + p // POINTS, p_index, r : r + 1, :]

            cols[8 * v + s] = dot_t(repeat, spread(row_of, 8)).astype(BF16) * diag[...]

    for v in range(5):
        if v < 4:
            build(v)
        if v > 0:
            expand_points(turned, cols, result, v - 1)
            for n, step in enumerate((0, 3)):
                row_copy(result, out, sem, n, step, v - 1).start()
    for v in range(4):
        for n, step in enumerate((0, 3)):
            row_copy(result, out, sem, n, step, v).wait()


def last_kernel(near, right, far, cols, turn_far, partial, out, pairs, picked, turned, result, scalars, sem):
    fetch = index_copy(near, scalars, sem)
    fetch.start()
    kc = lax.axis_index("kc")
    pair_blocks(lambda n: right[n], lambda n: far[n], pairs)
    turn = turn_far[...]
    fetch.wait()
    for v in range(5):
        if v < 4:
            turn_points(scalars, 256 * kc, pairs, turn, picked, turned, v)
        if v > 0:
            expand_points(turned, cols, result, v - 1)
            for n, step in enumerate((1, 2)):
                row_copy(result, out, sem, n, step, v - 1).start()
    for v in range(4):
        for n, step in enumerate((1, 2)):
            row_copy(result, out, sem, n, step, v).wait()


def call(kernel, outs, in_specs, out_specs, scratch, flops, aliases=None):
    return pl.pallas_call(
        kernel,
        out_shape=outs,
        in_specs=in_specs,
        out_specs=out_specs,
        scratch_shapes=scratch,
        input_output_aliases=aliases or {},
        compiler_params=pltpu.CompilerParams(vmem_limit_bytes=8 << 20),
        cost_estimate=pl.CostEstimate(flops=flops, bytes_accessed=flops // 10, transcendentals=0),
    )


def shape(*dims):
    return jax.ShapeDtypeStruct(dims, BF16)


def shift(value, by):
    return lax.ppermute(value, "kc", [(i, (i + by) % 4) for i in range(4)])


def partner(value):
    return lax.ppermute(value, "kf_2", [(0, 1), (1, 0)])


def shards(kernel_coarse, coefficients, nearest):
    other = partner(kernel_coarse)
    rotations = (128, 32, LANES)
    block = (PAIRS, LANES)
    table = jnp.pad(nearest.reshape(1, FINE), ((32, 15), (0, FINE))).astype(F32)
    rows = jnp.pad(coefficients.astype(F32), ((40, 4), (0, 2 * FINE - 2 * LANES)))
    fetched = jnp.pad(kernel_coarse.astype(F32), ((0, 16), (0, 0))) + table + rows
    scalars = [pltpu.SMEM((1, FINE), jnp.int32), pltpu.SemaphoreType.DMA((9,))]
    index = jax.ShapeDtypeStruct((1, FINE), jnp.int32)
    own_copies, near, slots, coef_own = call(
        own_kernel, (shape(*rotations), index, index, shape(8, LANES)), [VMEM], (VMEM,) * 4, [], 1000000
    )(fetched)
    packed = call(
        pack_kernel, shape(PEERS, 40, LANES), [VMEM] * 4, VMEM, [pltpu.VMEM(rotations, BF16)] + scalars, 1000000
    )(slots, own_copies, other, coef_own)
    received = lax.all_to_all(packed, ZY, split_axis=0, concat_axis=0, tiled=True)
    mine, up, down, across = call(
        split_kernel, tuple(shape(n, *block) for n in (64, 69, 69, 5)), [VMEM] * 2, (VMEM,) * 4, [], 100000
    )(received, coef_own)
    left = shift(up, 1)
    right = shift(down, -1)
    far_coef = shift(across, 2)
    far = shift(mine, 2)
    coef_half = call(collect_kernel, shape(16, *block), [VMEM] * 4, VMEM, [], 100000)(received, left, right, far_coef)
    coef_other = partner(coef_half)
    pairs = pltpu.VMEM((128, *block), BF16)
    picked = pltpu.VMEM((2, 1024, LANES), BF16)
    turned = pltpu.VMEM((LANES, 4096), BF16)
    rows_turned = call(
        turn_kernel, shape(LANES, 4096), [VMEM] * 4, VMEM, [pairs, picked] + scalars, 2000000
    )(near, mine, coef_own, left)
    partial, cols, turn_far = call(
        middle_kernel,
        (shape(256, 4096), shape(32, LANES, LANES), shape(LANES, LANES)),
        [VMEM] * 5,
        (ANY, VMEM, VMEM),
        [pltpu.VMEM((4, 8, *block), F32), pltpu.VMEM((LANES, LANES), BF16), turned] + scalars[1:],
        8000000,
    )(coef_half, coef_other, right, far_coef, rows_turned)
    return call(
        last_kernel,
        shape(256, 4096),
        [VMEM] * 5 + [ANY],
        ANY,
        [pairs, picked, turned, turned] + scalars,
        3000000,
        {5: 0},
    )(near, right, far, cols, turn_far, partial)


def solution(mesh):
    split = Mesh(mesh.devices.reshape(8, 4, 2, mesh.shape["kc"]), KF_KC)
    return jax.shard_map(
        shards,
        mesh=split,
        in_specs=(P(KF, None), P(KF_KC, None), P()),
        out_specs=P(KF, "kc"),
        check_vma=False,
    )
```

```python
import jax
import jax.numpy as jnp
from jax import lax
from jax.experimental import pallas as pl
from jax.experimental.pallas import tpu as pltpu
from jax.sharding import Mesh
from jax.sharding import PartitionSpec as P


KF = ("kf_0", "kf_1", "kf_2")
ZY = ("kf_0", "kf_1")
KF_KC = ("kf_0", "kf_1", "kf_2", "kc")
LANES = 128
PAIRS = 16
POINTS = 4
PEERS = 32
FINE = 1024
BF16 = jnp.bfloat16
F32 = jnp.float32
VMEM = pl.BlockSpec(memory_space=pltpu.VMEM)
SMEM = pl.BlockSpec(memory_space=pltpu.SMEM)
ANY = pl.BlockSpec(memory_space=pl.ANY)


def iota(shape, dim):
    return lax.broadcasted_iota(jnp.int32, shape, dim)


def dot_t(a, b):
    return lax.dot_general(a, b, (((1,), (1,)), ((), ())), preferred_element_type=F32)


def turn_rows(rows, copies):
    for b in range(16):
        block = rows[:32, b * LANES : (b + 1) * LANES].astype(F32)
        for s in range(8):
            turned = pltpu.roll(block, s * PAIRS, 1) if s else block
            copies[s * 16 + b] = turned.astype(BF16)


def halves_stacked(coef):
    return jnp.concatenate([coef[:, :LANES], coef[:, LANES:]], axis=0)


def own_kernel(fetched, copies, near, slots, coef):
    c = fetched[32:33, :FINE].astype(jnp.int32)
    near[...] = c
    slots[...] = ((iota((1, FINE), 1) % POINTS - c) & 7) * 16 + (c >> 3)
    coef[...] = halves_stacked(fetched[40:44, : 2 * LANES]).astype(BF16)
    turn_rows(fetched, copies)


def index_copy(near, scalars, sem):
    return pltpu.make_async_copy(near, scalars, sem.at[0])


def pack_kernel(slots, own_copies, other, coef_own, coef_other, out, other_copies, scalars, sem):
    fetch = index_copy(slots, scalars, sem)
    fetch.start()
    kc = lax.axis_index("kc")
    core = lax.axis_index("kf_2")
    turn_rows(other, other_copies)
    copies = (own_copies, other_copies)
    a = coef_own[...].astype(F32)
    o = halves_stacked(coef_other[...].astype(F32))
    coef = jnp.concatenate([jnp.where(core == 0, a, o), jnp.where(core == 0, o, a)], axis=0).astype(BF16)
    fetch.wait()
    group = iota((PAIRS, LANES), 1) // PAIRS
    base = 16 * core + 4 * kc

    def body(d, carry):
        tiles = [None, None]
        for j in range(POINTS):
            slot = scalars[0, 32 * d + base + j]
            for lo in range(2):
                for n in range(2):
                    piece = copies[n][slot ^ (64 * lo), lo * PAIRS : (lo + 1) * PAIRS, :]
                    tiles[n] = piece if tiles[n] is None else jnp.where(group == lo * POINTS + j, piece, tiles[n])
        out[d, pl.ds(pl.multiple_of(core * PAIRS, PAIRS), PAIRS), :] = tiles[0]
        out[d, pl.ds(pl.multiple_of((1 - core) * PAIRS, PAIRS), PAIRS), :] = tiles[1]
        out[d, 2 * PAIRS :, :] = coef
        return carry

    lax.fori_loop(0, PEERS, body, 0, unroll=4)


def row_block(received, n):
    return received[n // 2, n % 2 * PAIRS : (n % 2 + 1) * PAIRS, :]


def row_coefficients(coef_own):
    mine = coef_own[...].astype(F32)
    return jnp.concatenate([mine, mine], axis=0).astype(BF16)


def split_kernel(received, coef_own, mine, up, down, across):
    kc = lax.axis_index("kc")
    for n in range(64):
        block = row_block(received, n)
        for target in (mine, up, down):
            target[n] = block
    for step, target, at in ((1, up, 64), (3, down, 64), (2, across, 0)):
        first = (kc + step) % 4 * 8
        for p in range(8):
            target[at + p] = received[first + p, 2 * PAIRS :, :]
        target[at + 8] = row_coefficients(coef_own)


def spread(row_of, count):
    keep = iota((8, LANES), 1) // PAIRS == iota((8, LANES), 0)
    pieces = []
    for p in range(count):
        for half in range(2):
            pieces.append(jnp.where(keep, jnp.broadcast_to(row_of(p, half), (8, LANES)), 0.0))
    return jnp.concatenate(pieces, axis=0).astype(BF16)


def repeat_matrix():
    same = iota((LANES, LANES), 0) % PAIRS == iota((LANES, LANES), 1) % PAIRS
    return jnp.where(same, 1.0, 0.0).astype(BF16)


def pair_blocks(low_of, high_of, pairs):
    low = iota((PAIRS, LANES), 1) < 64
    for n in range(64):
        first, second = low_of(n), high_of(n)
        pairs[2 * n] = jnp.where(low, first, pltpu.roll(second.astype(F32), 64, 1).astype(BF16))
        pairs[2 * n + 1] = jnp.where(low, pltpu.roll(first.astype(F32), 64, 1).astype(BF16), second)


def turn_points(scalars, first, pairs, turn, picked, turned, v):
    for i in range(64):
        picked[v % 2, i * PAIRS : (i + 1) * PAIRS, :] = pairs[scalars[0, first + 64 * v + i]]
    turned[:, v * 1024 : (v + 1) * 1024] = dot_t(turn, picked[v % 2]).astype(BF16)


def expand_points(turned, cols, result, v):
    for u in range(8 * v, 8 * v + 8):
        at = slice(u * LANES, (u + 1) * LANES)
        result[:, at] = jnp.dot(turned[:, at], cols[u], preferred_element_type=F32).astype(BF16)


def row_copy(result, out, sem, n, step, v):
    row = pl.multiple_of((lax.axis_index("kc") + step) % 4 * 64, 64)
    at = pl.ds(v * 1024, 1024)
    return pltpu.make_async_copy(result.at[pl.ds(n * 64, 64), at], out.at[pl.ds(row, 64), at], sem.at[1 + 4 * n + v])


def diagonal():
    same = iota((LANES, LANES), 0) // PAIRS == iota((LANES, LANES), 1) // PAIRS
    return jnp.where(same, 1.0, 0.0).astype(BF16)


def turn_of(first, second, repeat, diag):
    rows = (first.astype(F32), second.astype(F32))

    def row_of(p, half):
        at = half * POINTS + p % POINTS
        return rows[p // POINTS][at : at + 1]

    return jnp.dot(spread(row_of, 8), repeat, preferred_element_type=F32).astype(BF16) * diag


def middle_kernel(
    near, received, mine, coef_own, left, right, far_coef, out, cols, turn_far,
    pieces, pairs, diag, picked, turned, result, scalars, sem
):
    fetch = index_copy(near, scalars, sem)
    fetch.start()
    kc = lax.axis_index("kc")
    repeat = repeat_matrix()
    diag[...] = diagonal()
    turn = turn_of(coef_own[...], left[72], repeat, diag[...])
    turn_far[...] = turn_of(right[72], far_coef[8], repeat, diag[...])
    for p in range(8):
        pieces[kc, p] = received[kc * 8 + p, 2 * PAIRS :, :].astype(F32)
        pieces[(kc + 3) % 4, p] = left[64 + p].astype(F32)
        pieces[(kc + 1) % 4, p] = right[64 + p].astype(F32)
        pieces[(kc + 2) % 4, p] = far_coef[p].astype(F32)
    pair_blocks(lambda n: mine[n], lambda n: left[n], pairs)

    def build(v):
        for s in range(8):
            p_index, h, par = 2 * v + s // 4, s // 2 % 2, s % 2

            def row_of(p, half):
                r = h * 8 + half * POINTS + p % POINTS
                return pieces[par * 2 + p // POINTS, p_index, r : r + 1, :]

            cols[8 * v + s] = dot_t(repeat, spread(row_of, 8)).astype(BF16) * diag[...]

    build(0)
    fetch.wait()
    for v in range(5):
        if v < 4:
            turn_points(scalars, 256 * kc, pairs, turn, picked, turned, v)
            if v > 0:
                build(v)
        if v > 0:
            expand_points(turned, cols, result, v - 1)
            for n, step in enumerate((0, 3)):
                row_copy(result, out, sem, n, step, v - 1).start()
    for v in range(4):
        for n, step in enumerate((0, 3)):
            row_copy(result, out, sem, n, step, v).wait()


def last_kernel(near, right, far, cols, turn_far, partial, out, pairs, picked, turned, result, scalars, sem):
    fetch = index_copy(near, scalars, sem)
    fetch.start()
    kc = lax.axis_index("kc")
    pair_blocks(lambda n: right[n], lambda n: far[n], pairs)
    turn = turn_far[...]
    fetch.wait()
    for v in range(5):
        if v < 4:
            turn_points(scalars, 256 * kc, pairs, turn, picked, turned, v)
        if v > 0:
            expand_points(turned, cols, result, v - 1)
            for n, step in enumerate((1, 2)):
                row_copy(result, out, sem, n, step, v - 1).start()
    for v in range(4):
        for n, step in enumerate((1, 2)):
            row_copy(result, out, sem, n, step, v).wait()


def call(kernel, outs, in_specs, out_specs, scratch, flops, aliases=None):
    return pl.pallas_call(
        kernel,
        out_shape=outs,
        in_specs=in_specs,
        out_specs=out_specs,
        scratch_shapes=scratch,
        input_output_aliases=aliases or {},
        compiler_params=pltpu.CompilerParams(vmem_limit_bytes=8 << 20),
        cost_estimate=pl.CostEstimate(flops=flops, bytes_accessed=flops // 10, transcendentals=0),
    )


def shape(*dims):
    return jax.ShapeDtypeStruct(dims, BF16)


def shift(value, by):
    return lax.ppermute(value, "kc", [(i, (i + by) % 4) for i in range(4)])


def partner(value):
    return lax.ppermute(value, "kf_2", [(0, 1), (1, 0)])


def shards(kernel_coarse, coefficients, nearest):
    other = partner(kernel_coarse)
    coef_other = partner(coefficients)
    rotations = (128, 32, LANES)
    block = (PAIRS, LANES)
    table = jnp.pad(nearest.reshape(1, FINE), ((32, 15), (0, FINE))).astype(F32)
    rows = jnp.pad(coefficients.astype(F32), ((40, 4), (0, 2 * FINE - 2 * LANES)))
    fetched = jnp.pad(kernel_coarse.astype(F32), ((0, 16), (0, 0))) + table + rows
    scalars = [pltpu.SMEM((1, FINE), jnp.int32), pltpu.SemaphoreType.DMA((9,))]
    index = jax.ShapeDtypeStruct((1, FINE), jnp.int32)
    own_copies, near, slots, coef_own = call(
        own_kernel, (shape(*rotations), index, index, shape(8, LANES)), [VMEM], (VMEM,) * 4, [], 1000000
    )(fetched)
    packed = call(
        pack_kernel, shape(PEERS, 48, LANES), [VMEM] * 5, VMEM, [pltpu.VMEM(rotations, BF16)] + scalars, 1000000
    )(slots, own_copies, other, coef_own, coef_other)
    received = lax.all_to_all(packed, ZY, split_axis=0, concat_axis=0, tiled=True)
    mine, up, down, across = call(
        split_kernel, tuple(shape(n, *block) for n in (64, 73, 73, 9)), [VMEM] * 2, (VMEM,) * 4, [], 100000
    )(received, coef_own)
    left = shift(up, 1)
    right = shift(down, -1)
    far_coef = shift(across, 2)
    far = shift(mine, 2)
    pairs = pltpu.VMEM((128, *block), BF16)
    picked = pltpu.VMEM((2, 1024, LANES), BF16)
    turned = pltpu.VMEM((LANES, 4096), BF16)
    partial, cols, turn_far = call(
        middle_kernel,
        (shape(256, 4096), shape(32, LANES, LANES), shape(LANES, LANES)),
        [VMEM] * 7,
        (ANY, VMEM, VMEM),
        [pltpu.VMEM((4, 8, *block), F32), pairs, pltpu.VMEM((LANES, LANES), BF16), picked, turned, turned] + scalars,
        8000000,
    )(near, received, mine, coef_own, left, right, far_coef)
    return call(
        last_kernel,
        shape(256, 4096),
        [VMEM] * 5 + [ANY],
        ANY,
        [pairs, picked, turned, turned] + scalars,
        3000000,
        {5: 0},
    )(near, right, far, cols, turn_far, partial)


def solution(mesh):
    split = Mesh(mesh.devices.reshape(8, 4, 2, mesh.shape["kc"]), KF_KC)
    return jax.shard_map(
        shards,
        mesh=split,
        in_specs=(P(KF, None), P(KF_KC, None), P()),
        out_specs=P(KF, "kc"),
        check_vma=False,
    )
```

```python
import jax
import jax.numpy as jnp
from jax import lax
from jax.experimental import pallas as pl
from jax.experimental.pallas import tpu as pltpu
from jax.sharding import Mesh
from jax.sharding import PartitionSpec as P


KF = ("kf_0", "kf_1", "kf_2")
ZY = ("kf_0", "kf_1")
KF_KC = ("kf_0", "kf_1", "kf_2", "kc")
LANES = 128
PAIRS = 16
POINTS = 4
PEERS = 32
FINE = 1024
BF16 = jnp.bfloat16
F32 = jnp.float32
VMEM = pl.BlockSpec(memory_space=pltpu.VMEM)
SMEM = pl.BlockSpec(memory_space=pltpu.SMEM)
ANY = pl.BlockSpec(memory_space=pl.ANY)


def iota(shape, dim):
    return lax.broadcasted_iota(jnp.int32, shape, dim)


def dot_t(a, b):
    return lax.dot_general(a, b, (((1,), (1,)), ((), ())), preferred_element_type=F32)


def turn_rows(rows, copies):
    for b in range(16):
        block = rows[:32, b * LANES : (b + 1) * LANES].astype(F32)
        for s in range(8):
            turned = pltpu.roll(block, s * PAIRS, 1) if s else block
            copies[s * 16 + b] = turned.astype(BF16)


def halves_stacked(coef):
    return jnp.concatenate([coef[:, :LANES], coef[:, LANES:]], axis=0)


def own_kernel(fetched, copies, near, slots, coef):
    c = fetched[32:33, :FINE].astype(jnp.int32)
    near[...] = c
    slots[...] = ((iota((1, FINE), 1) % POINTS - c) & 7) * 16 + (c >> 3)
    coef[...] = halves_stacked(fetched[40:44, : 2 * LANES]).astype(BF16)
    turn_rows(fetched, copies)


def index_copy(near, scalars, sem):
    return pltpu.make_async_copy(near, scalars, sem.at[0])


def pack_kernel(slots, own_copies, other, coef, out, other_copies, scalars, sem):
    fetch = index_copy(slots, scalars, sem)
    fetch.start()
    kc = lax.axis_index("kc")
    core = lax.axis_index("kf_2")
    turn_rows(other, other_copies)
    copies = (own_copies, other_copies)
    fetch.wait()
    group = iota((PAIRS, LANES), 1) // PAIRS
    base = 16 * core + 4 * kc

    def body(d, carry):
        tiles = [None, None]
        for j in range(POINTS):
            slot = scalars[0, 32 * d + base + j]
            for lo in range(2):
                for n in range(2):
                    piece = copies[n][slot ^ (64 * lo), lo * PAIRS : (lo + 1) * PAIRS, :]
                    tiles[n] = piece if tiles[n] is None else jnp.where(group == lo * POINTS + j, piece, tiles[n])
        out[d, pl.ds(pl.multiple_of(core * PAIRS, PAIRS), PAIRS), :] = tiles[0]
        out[d, pl.ds(pl.multiple_of((1 - core) * PAIRS, PAIRS), PAIRS), :] = tiles[1]
        out[d, 2 * PAIRS :, :] = coef[...]
        return carry

    lax.fori_loop(0, PEERS, body, 0, unroll=4)


def row_block(received, n):
    return received[n // 2, n % 2 * PAIRS : (n % 2 + 1) * PAIRS, :]


def row_coefficients(coef_own):
    mine = coef_own[...].astype(F32)
    return jnp.concatenate([mine, mine], axis=0).astype(BF16)


def put_pieces(received, kc, target, at):
    for p in range(8):
        target[at + p // 2, p % 2 * 8 : p % 2 * 8 + 8, :] = received[kc * 8 + p, 2 * PAIRS :, :]


def split_kernel(received, coef_own, up_1, up_2, down_1, down_2, across):
    kc = lax.axis_index("kc")
    mine = row_coefficients(coef_own)
    for n in range(32):
        up_1[n] = row_block(received, n)
        down_2[n] = row_block(received, n)
        up_2[n] = row_block(received, 32 + n)
        down_1[n] = row_block(received, 32 + n)
    for step, target, at in ((1, up_1, 32), (3, down_1, 32), (2, across, 0)):
        put_pieces(received, (kc + step) % 4, target, at)
        target[at + 4] = mine


def collect_kernel(received, left_1, right_1, far_coef, collected):
    put_pieces(received, lax.axis_index("kc"), collected, 0)
    for n in range(4):
        collected[4 + n] = left_1[32 + n]
        collected[8 + n] = right_1[32 + n]
        collected[12 + n] = far_coef[n]


def spread(row_of, count):
    keep = iota((8, LANES), 1) // PAIRS == iota((8, LANES), 0)
    pieces = []
    for p in range(count):
        for half in range(2):
            pieces.append(jnp.where(keep, jnp.broadcast_to(row_of(p, half), (8, LANES)), 0.0))
    return jnp.concatenate(pieces, axis=0).astype(BF16)


def repeat_matrix():
    same = iota((LANES, LANES), 0) % PAIRS == iota((LANES, LANES), 1) % PAIRS
    return jnp.where(same, 1.0, 0.0).astype(BF16)


def pair_blocks(low_of, high_of, pairs):
    low = iota((PAIRS, LANES), 1) < 64
    for n in range(64):
        first, second = low_of(n), high_of(n)
        pairs[2 * n] = jnp.where(low, first, pltpu.roll(second.astype(F32), 64, 1).astype(BF16))
        pairs[2 * n + 1] = jnp.where(low, pltpu.roll(first.astype(F32), 64, 1).astype(BF16), second)


def turn_points(scalars, first, pairs, turn, picked, turned, v):
    for i in range(64):
        picked[v % 2, i * PAIRS : (i + 1) * PAIRS, :] = pairs[scalars[0, first + 64 * v + i]]
    turned[:, v * 1024 : (v + 1) * 1024] = dot_t(turn, picked[v % 2]).astype(BF16)


def expand_points(turned, cols, result, v):
    for u in range(8 * v, 8 * v + 8):
        at = slice(u * LANES, (u + 1) * LANES)
        result[:, at] = jnp.dot(turned[:, at], cols[u], preferred_element_type=F32).astype(BF16)


def row_copy(result, out, sem, n, step, v):
    row = pl.multiple_of((lax.axis_index("kc") + step) % 4 * 64, 64)
    at = pl.ds(v * 1024, 1024)
    return pltpu.make_async_copy(result.at[pl.ds(n * 64, 64), at], out.at[pl.ds(row, 64), at], sem.at[1 + 4 * n + v])


def diagonal():
    same = iota((LANES, LANES), 0) // PAIRS == iota((LANES, LANES), 1) // PAIRS
    return jnp.where(same, 1.0, 0.0).astype(BF16)


def turn_of(first, second, repeat, diag):
    rows = (first.astype(F32), second.astype(F32))

    def row_of(p, half):
        at = half * POINTS + p % POINTS
        return rows[p // POINTS][at : at + 1]

    return jnp.dot(spread(row_of, 8), repeat, preferred_element_type=F32).astype(BF16) * diag


def turn_kernel(near, received, coef_own, left_1, left_2, turned, pairs, picked, scalars, sem):
    fetch = index_copy(near, scalars, sem)
    fetch.start()
    kc = lax.axis_index("kc")
    turn = turn_of(coef_own[...], left_1[36], repeat_matrix(), diagonal())
    pair_blocks(
        lambda n: row_block(received, n), lambda n: left_1[n] if n < 32 else left_2[n - 32], pairs
    )
    fetch.wait()
    for v in range(4):
        turn_points(scalars, 256 * kc, pairs, turn, picked, turned, v)


def middle_kernel(
    coef_half, coef_other, right_1, far_coef, turned, out, cols, turn_far, pieces, diag, result, sem
):
    kc = lax.axis_index("kc")
    repeat = repeat_matrix()
    diag[...] = diagonal()
    turn_far[...] = turn_of(right_1[36], far_coef[4], repeat, diag[...])
    core = lax.axis_index("kf_2")
    for n, step in enumerate((0, 3, 1, 2)):
        for p in range(8):
            for owner, source in ((core, coef_half), (1 - core, coef_other)):
                piece = source[4 * n + p // 2, p % 2 * 8 : p % 2 * 8 + 8, :].astype(F32)
                pieces[(kc + step) % 4, p, pl.ds(pl.multiple_of(owner * 8, 8), 8), :] = piece

    def build(v):
        for s in range(8):
            p_index, h, par = 2 * v + s // 4, s // 2 % 2, s % 2

            def row_of(p, half):
                r = h * 8 + half * POINTS + p % POINTS
                return pieces[par * 2 + p // POINTS, p_index, r : r + 1, :]

            cols[8 * v + s] = dot_t(repeat, spread(row_of, 8)).astype(BF16) * diag[...]

    for v in range(5):
        if v < 4:
            build(v)
        if v > 0:
            expand_points(turned, cols, result, v - 1)
            for n, step in enumerate((0, 3)):
                row_copy(result, out, sem, n, step, v - 1).start()
    for v in range(4):
        for n, step in enumerate((0, 3)):
            row_copy(result, out, sem, n, step, v).wait()


def last_kernel(near, right_1, right_2, far_1, far_2, cols, turn_far, partial, out, pairs, picked, turned, result, scalars, sem):
    fetch = index_copy(near, scalars, sem)
    fetch.start()
    kc = lax.axis_index("kc")
    pair_blocks(
        lambda n: right_2[n] if n < 32 else right_1[n - 32], lambda n: far_1[n] if n < 32 else far_2[n - 32], pairs
    )
    turn = turn_far[...]
    fetch.wait()
    for v in range(5):
        if v < 4:
            turn_points(scalars, 256 * kc, pairs, turn, picked, turned, v)
        if v > 0:
            expand_points(turned, cols, result, v - 1)
            for n, step in enumerate((1, 2)):
                row_copy(result, out, sem, n, step, v - 1).start()
    for v in range(4):
        for n, step in enumerate((1, 2)):
            row_copy(result, out, sem, n, step, v).wait()


def call(kernel, outs, in_specs, out_specs, scratch, flops, aliases=None):
    return pl.pallas_call(
        kernel,
        out_shape=outs,
        in_specs=in_specs,
        out_specs=out_specs,
        scratch_shapes=scratch,
        input_output_aliases=aliases or {},
        compiler_params=pltpu.CompilerParams(vmem_limit_bytes=8 << 20),
        cost_estimate=pl.CostEstimate(flops=flops, bytes_accessed=flops // 10, transcendentals=0),
    )


def shape(*dims):
    return jax.ShapeDtypeStruct(dims, BF16)


def shift(value, by):
    return lax.ppermute(value, "kc", [(i, (i + by) % 4) for i in range(4)])


def partner(value):
    return lax.ppermute(value, "kf_2", [(0, 1), (1, 0)])


def shards(kernel_coarse, coefficients, nearest):
    other = partner(kernel_coarse)
    rotations = (128, 32, LANES)
    block = (PAIRS, LANES)
    table = jnp.pad(nearest.reshape(1, FINE), ((32, 15), (0, FINE))).astype(F32)
    rows = jnp.pad(coefficients.astype(F32), ((40, 4), (0, 2 * FINE - 2 * LANES)))
    fetched = jnp.pad(kernel_coarse.astype(F32), ((0, 16), (0, 0))) + table + rows
    scalars = [pltpu.SMEM((1, FINE), jnp.int32), pltpu.SemaphoreType.DMA((9,))]
    index = jax.ShapeDtypeStruct((1, FINE), jnp.int32)
    own_copies, near, slots, coef_own = call(
        own_kernel, (shape(*rotations), index, index, shape(8, LANES)), [VMEM], (VMEM,) * 4, [], 1000000
    )(fetched)
    packed = call(
        pack_kernel, shape(PEERS, 40, LANES), [VMEM] * 4, VMEM, [pltpu.VMEM(rotations, BF16)] + scalars, 1000000
    )(slots, own_copies, other, coef_own)
    received = lax.all_to_all(packed, ZY, split_axis=0, concat_axis=0, tiled=True)
    sizes = (37, 32, 37, 32, 5)
    up_1, up_2, down_1, down_2, across = call(
        split_kernel, tuple(shape(n, *block) for n in sizes), [VMEM] * 2, (VMEM,) * 5, [], 100000
    )(received, coef_own)
    left_1 = shift(up_1, 1)
    right_1 = shift(down_1, -1)
    far_coef = shift(across, 2)
    left_2 = shift(up_2, 1)
    right_2 = shift(down_2, -1)
    far_1 = shift(left_1[:PEERS], 1)
    far_2 = shift(right_1[:PEERS], -1)
    coef_half = call(collect_kernel, shape(16, *block), [VMEM] * 4, VMEM, [], 100000)(received, left_1, right_1, far_coef)
    coef_other = partner(coef_half)
    pairs = pltpu.VMEM((128, *block), BF16)
    picked = pltpu.VMEM((2, 1024, LANES), BF16)
    turned = pltpu.VMEM((LANES, 4096), BF16)
    rows_turned = call(
        turn_kernel, shape(LANES, 4096), [VMEM] * 5, VMEM, [pairs, picked] + scalars, 2000000
    )(near, received, coef_own, left_1, left_2)
    partial, cols, turn_far = call(
        middle_kernel,
        (shape(256, 4096), shape(32, LANES, LANES), shape(LANES, LANES)),
        [VMEM] * 5,
        (ANY, VMEM, VMEM),
        [pltpu.VMEM((4, 8, *block), F32), pltpu.VMEM((LANES, LANES), BF16), turned] + scalars[1:],
        8000000,
    )(coef_half, coef_other, right_1, far_coef, rows_turned)
    return call(
        last_kernel,
        shape(256, 4096),
        [VMEM] * 7 + [ANY],
        ANY,
        [pairs, picked, turned, turned] + scalars,
        3000000,
        {7: 0},
    )(near, right_1, right_2, far_1, far_2, cols, turn_far, partial)


def solution(mesh):
    split = Mesh(mesh.devices.reshape(8, 4, 2, mesh.shape["kc"]), KF_KC)
    return jax.shard_map(
        shards,
        mesh=split,
        in_specs=(P(KF, None), P(KF_KC, None), P()),
        out_specs=P(KF, "kc"),
        check_vma=False,
    )
```

```python
import jax
import jax.numpy as jnp
from jax import lax
from jax.experimental import pallas as pl
from jax.experimental.pallas import tpu as pltpu
from jax.sharding import Mesh
from jax.sharding import PartitionSpec as P


KF = ("kf_0", "kf_1", "kf_2")
ZY = ("kf_0", "kf_1")
KF_KC = ("kf_0", "kf_1", "kf_2", "kc")
LANES = 128
PAIRS = 16
POINTS = 4
PEERS = 32
RISING = 44
FINE = 1024
BF16 = jnp.bfloat16
F32 = jnp.float32
VMEM = pl.BlockSpec(memory_space=pltpu.VMEM)
SMEM = pl.BlockSpec(memory_space=pltpu.SMEM)
ANY = pl.BlockSpec(memory_space=pl.ANY)


def iota(shape, dim):
    return lax.broadcasted_iota(jnp.int32, shape, dim)


def dot_t(a, b):
    return lax.dot_general(a, b, (((1,), (1,)), ((), ())), preferred_element_type=F32)


def turn_rows(rows, copies):
    for b in range(16):
        block = rows[:32, b * LANES : (b + 1) * LANES].astype(F32)
        for s in range(8):
            turned = pltpu.roll(block, s * PAIRS, 1) if s else block
            copies[s * 16 + b] = turned.astype(BF16)


def halves_stacked(coef):
    return jnp.concatenate([coef[:, :LANES], coef[:, LANES:]], axis=0)


def index_copy(near, scalars, sem):
    return pltpu.make_async_copy(near, scalars, sem.at[0])


def pack_kernel(fetched, other, out, near, coef, own_copies, other_copies, slots, scalars, sem):
    c = fetched[32:33, :FINE].astype(jnp.int32)
    slots[...] = ((iota((1, FINE), 1) % POINTS - c) & 7) * 16 + (c >> 3)
    fetch = index_copy(slots, scalars, sem)
    fetch.start()
    near[...] = c
    coef[...] = halves_stacked(fetched[40:44, : 2 * LANES]).astype(BF16)
    kc = lax.axis_index("kc")
    core = lax.axis_index("kf_2")
    turn_rows(fetched, own_copies)
    turn_rows(other, other_copies)
    copies = (own_copies, other_copies)
    fetch.wait()
    group = iota((PAIRS, LANES), 1) // PAIRS
    base = 16 * core + 4 * kc

    def body(d, carry):
        tiles = [None, None]
        for j in range(POINTS):
            slot = scalars[0, 32 * d + base + j]
            for lo in range(2):
                for n in range(2):
                    piece = copies[n][slot ^ (64 * lo), lo * PAIRS : (lo + 1) * PAIRS, :]
                    tiles[n] = piece if tiles[n] is None else jnp.where(group == lo * POINTS + j, piece, tiles[n])
        out[d, pl.ds(pl.multiple_of(core * PAIRS, PAIRS), PAIRS), :] = tiles[0]
        out[d, pl.ds(pl.multiple_of((1 - core) * PAIRS, PAIRS), PAIRS), :] = tiles[1]
        out[d, 2 * PAIRS :, :] = coef[...]
        return carry

    lax.fori_loop(0, PEERS, body, 0, unroll=4)


def row_block(received, n):
    return received[n // 2, n % 2 * PAIRS : (n % 2 + 1) * PAIRS, :]


def row_coefficients(coef_own):
    mine = coef_own[...].astype(F32)
    return jnp.concatenate([mine, mine], axis=0).astype(BF16)


def put_pieces(received, kc, target, at):
    for p in range(8):
        target[at + p // 2, p % 2 * 8 : p % 2 * 8 + 8, :] = received[kc * 8 + p, 2 * PAIRS :, :]


def split_kernel(received, coef_own, up_1, up_2, down_1, down_2, across):
    kc = lax.axis_index("kc")
    mine = row_coefficients(coef_own)
    for n in range(64):
        block = row_block(received, n)
        if n < RISING:
            up_1[n] = block
            down_2[n] = block
        else:
            up_2[n - RISING] = block
            down_1[n - RISING] = block
    for step, target, at in ((1, up_1, RISING), (3, down_1, 64 - RISING), (2, across, 0)):
        put_pieces(received, (kc + step) % 4, target, at)
        target[at + 4] = mine


def collect_kernel(received, left_1, right_1, far_coef, collected):
    put_pieces(received, lax.axis_index("kc"), collected, 0)
    for n in range(4):
        collected[4 + n] = left_1[RISING + n]
        collected[8 + n] = right_1[64 - RISING + n]
        collected[12 + n] = far_coef[n]


def spread(row_of, count):
    keep = iota((8, LANES), 1) // PAIRS == iota((8, LANES), 0)
    pieces = []
    for p in range(count):
        for half in range(2):
            pieces.append(jnp.where(keep, jnp.broadcast_to(row_of(p, half), (8, LANES)), 0.0))
    return jnp.concatenate(pieces, axis=0).astype(BF16)


def repeat_matrix():
    same = iota((LANES, LANES), 0) % PAIRS == iota((LANES, LANES), 1) % PAIRS
    return jnp.where(same, 1.0, 0.0).astype(BF16)


def pair_blocks(low_of, high_of, pairs):
    low = iota((PAIRS, LANES), 1) < 64
    for n in range(64):
        first, second = low_of(n), high_of(n)
        pairs[2 * n] = jnp.where(low, first, pltpu.roll(second.astype(F32), 64, 1).astype(BF16))
        pairs[2 * n + 1] = jnp.where(low, pltpu.roll(first.astype(F32), 64, 1).astype(BF16), second)


def turn_points(scalars, first, pairs, turn, picked, turned, v):
    for i in range(64):
        picked[v % 2, i * PAIRS : (i + 1) * PAIRS, :] = pairs[scalars[0, first + 64 * v + i]]
    turned[:, v * 1024 : (v + 1) * 1024] = dot_t(turn, picked[v % 2]).astype(BF16)


def expand_points(turned, cols, result, v):
    for u in range(8 * v, 8 * v + 8):
        at = slice(u * LANES, (u + 1) * LANES)
        result[:, at] = jnp.dot(turned[:, at], cols[u], preferred_element_type=F32).astype(BF16)


def row_copy(result, out, sem, n, step, v):
    row = pl.multiple_of((lax.axis_index("kc") + step) % 4 * 64, 64)
    at = pl.ds(v * 1024, 1024)
    return pltpu.make_async_copy(result.at[pl.ds(n * 64, 64), at], out.at[pl.ds(row, 64), at], sem.at[1 + 4 * n + v])


def diagonal():
    same = iota((LANES, LANES), 0) // PAIRS == iota((LANES, LANES), 1) // PAIRS
    return jnp.where(same, 1.0, 0.0).astype(BF16)


def turn_of(first, second, repeat, diag):
    rows = (first.astype(F32), second.astype(F32))

    def row_of(p, half):
        at = half * POINTS + p % POINTS
        return rows[p // POINTS][at : at + 1]

    return jnp.dot(spread(row_of, 8), repeat, preferred_element_type=F32).astype(BF16) * diag


def turn_kernel(near, received, coef_own, left_1, left_2, turned, pairs, picked, scalars, sem):
    fetch = index_copy(near, scalars, sem)
    fetch.start()
    kc = lax.axis_index("kc")
    turn = turn_of(coef_own[...], left_1[RISING + 4], repeat_matrix(), diagonal())
    pair_blocks(
        lambda n: row_block(received, n), lambda n: left_1[n] if n < RISING else left_2[n - RISING], pairs
    )
    fetch.wait()
    for v in range(4):
        turn_points(scalars, 256 * kc, pairs, turn, picked, turned, v)


def middle_kernel(
    coef_half, coef_other, right_1, far_coef, turned, out, cols, turn_far, pieces, diag, result, sem
):
    kc = lax.axis_index("kc")
    repeat = repeat_matrix()
    diag[...] = diagonal()
    turn_far[...] = turn_of(right_1[68 - RISING], far_coef[4], repeat, diag[...])
    core = lax.axis_index("kf_2")
    for n, step in enumerate((0, 3, 1, 2)):
        for p in range(8):
            for owner, source in ((core, coef_half), (1 - core, coef_other)):
                piece = source[4 * n + p // 2, p % 2 * 8 : p % 2 * 8 + 8, :].astype(F32)
                pieces[(kc + step) % 4, p, pl.ds(pl.multiple_of(owner * 8, 8), 8), :] = piece

    def build(v):
        for s in range(8):
            p_index, h, par = 2 * v + s // 4, s // 2 % 2, s % 2

            def row_of(p, half):
                r = h * 8 + half * POINTS + p % POINTS
                return pieces[par * 2 + p // POINTS, p_index, r : r + 1, :]

            cols[8 * v + s] = dot_t(repeat, spread(row_of, 8)).astype(BF16) * diag[...]

    for v in range(5):
        if v < 4:
            build(v)
        if v > 0:
            expand_points(turned, cols, result, v - 1)
            for n, step in enumerate((0, 3)):
                row_copy(result, out, sem, n, step, v - 1).start()
    for v in range(4):
        for n, step in enumerate((0, 3)):
            row_copy(result, out, sem, n, step, v).wait()


def last_kernel(near, right_1, right_2, far_1, far_2, cols, turn_far, partial, out, pairs, picked, turned, result, scalars, sem):
    fetch = index_copy(near, scalars, sem)
    fetch.start()
    kc = lax.axis_index("kc")
    pair_blocks(
        lambda n: right_2[n] if n < RISING else right_1[n - RISING],
        lambda n: far_1[n] if n < RISING else far_2[n - RISING],
        pairs,
    )
    turn = turn_far[...]
    fetch.wait()
    for v in range(5):
        if v < 4:
            turn_points(scalars, 256 * kc, pairs, turn, picked, turned, v)
        if v > 0:
            expand_points(turned, cols, result, v - 1)
            for n, step in enumerate((1, 2)):
                row_copy(result, out, sem, n, step, v - 1).start()
    for v in range(4):
        for n, step in enumerate((1, 2)):
            row_copy(result, out, sem, n, step, v).wait()


def call(kernel, outs, in_specs, out_specs, scratch, flops, aliases=None):
    return pl.pallas_call(
        kernel,
        out_shape=outs,
        in_specs=in_specs,
        out_specs=out_specs,
        scratch_shapes=scratch,
        input_output_aliases=aliases or {},
        compiler_params=pltpu.CompilerParams(vmem_limit_bytes=8 << 20),
        cost_estimate=pl.CostEstimate(flops=flops, bytes_accessed=flops // 10, transcendentals=0),
    )


def shape(*dims):
    return jax.ShapeDtypeStruct(dims, BF16)


def shift(value, by):
    return lax.ppermute(value, "kc", [(i, (i + by) % 4) for i in range(4)])


def partner(value):
    return lax.ppermute(value, "kf_2", [(0, 1), (1, 0)])


def shards(kernel_coarse, coefficients, nearest):
    other = partner(kernel_coarse)
    rotations = (128, 32, LANES)
    block = (PAIRS, LANES)
    table = jnp.pad(nearest.reshape(1, FINE), ((32, 15), (0, FINE))).astype(F32)
    rows = jnp.pad(coefficients.astype(F32), ((40, 4), (0, 2 * FINE - 2 * LANES)))
    fetched = jnp.pad(kernel_coarse.astype(F32), ((0, 16), (0, 0))) + table + rows
    scalars = [pltpu.SMEM((1, FINE), jnp.int32), pltpu.SemaphoreType.DMA((9,))]
    copies = pltpu.VMEM(rotations, BF16)
    packed, near, coef_own = call(
        pack_kernel,
        (shape(PEERS, 40, LANES), jax.ShapeDtypeStruct((1, FINE), jnp.int32), shape(8, LANES)),
        [VMEM] * 2,
        (VMEM,) * 3,
        [copies, copies, pltpu.VMEM((1, FINE), jnp.int32)] + scalars,
        1000000,
    )(fetched, other)
    received = lax.all_to_all(packed, ZY, split_axis=0, concat_axis=0, tiled=True)
    sizes = (RISING + 5, 64 - RISING, 69 - RISING, RISING, 5)
    up_1, up_2, down_1, down_2, across = call(
        split_kernel, tuple(shape(n, *block) for n in sizes), [VMEM] * 2, (VMEM,) * 5, [], 100000
    )(received, coef_own)
    left_1 = shift(up_1, 1)
    right_1 = shift(down_1, -1)
    far_coef = shift(across, 2)
    left_2 = shift(up_2, 1)
    right_2 = shift(down_2, -1)
    far_1 = shift(left_1[:RISING], 1)
    far_2 = shift(right_1[: 64 - RISING], -1)
    coef_half = call(collect_kernel, shape(16, *block), [VMEM] * 4, VMEM, [], 100000)(received, left_1, right_1, far_coef)
    coef_other = partner(coef_half)
    pairs = pltpu.VMEM((128, *block), BF16)
    picked = pltpu.VMEM((2, 1024, LANES), BF16)
    turned = pltpu.VMEM((LANES, 4096), BF16)
    rows_turned = call(
        turn_kernel, shape(LANES, 4096), [VMEM] * 5, VMEM, [pairs, picked] + scalars, 2000000
    )(near, received, coef_own, left_1, left_2)
    partial, cols, turn_far = call(
        middle_kernel,
        (shape(256, 4096), shape(32, LANES, LANES), shape(LANES, LANES)),
        [VMEM] * 5,
        (ANY, VMEM, VMEM),
        [pltpu.VMEM((4, 8, *block), F32), pltpu.VMEM((LANES, LANES), BF16), turned] + scalars[1:],
        8000000,
    )(coef_half, coef_other, right_1, far_coef, rows_turned)
    return call(
        last_kernel,
        shape(256, 4096),
        [VMEM] * 7 + [ANY],
        ANY,
        [pairs, picked, turned, turned] + scalars,
        3000000,
        {7: 0},
    )(near, right_1, right_2, far_1, far_2, cols, turn_far, partial)


def solution(mesh):
    split = Mesh(mesh.devices.reshape(8, 4, 2, mesh.shape["kc"]), KF_KC)
    return jax.shard_map(
        shards,
        mesh=split,
        in_specs=(P(KF, None), P(KF_KC, None), P()),
        out_specs=P(KF, "kc"),
        check_vma=False,
    )
```

```python
import jax
import jax.numpy as jnp
from jax import lax
from jax.experimental import pallas as pl
from jax.experimental.pallas import tpu as pltpu
from jax.sharding import Mesh
from jax.sharding import PartitionSpec as P


KF = ("kf_0", "kf_1", "kf_2")
ZY = ("kf_0", "kf_1")
KF_KC = ("kf_0", "kf_1", "kf_2", "kc")
LANES = 128
PAIRS = 16
POINTS = 4
PEERS = 32
RISING = 40
FINE = 1024
BF16 = jnp.bfloat16
F32 = jnp.float32
VMEM = pl.BlockSpec(memory_space=pltpu.VMEM)
SMEM = pl.BlockSpec(memory_space=pltpu.SMEM)
ANY = pl.BlockSpec(memory_space=pl.ANY)


def iota(shape, dim):
    return lax.broadcasted_iota(jnp.int32, shape, dim)


def dot_t(a, b):
    return lax.dot_general(a, b, (((1,), (1,)), ((), ())), preferred_element_type=F32)


def turn_rows(rows, copies):
    for b in range(16):
        block = rows[:32, b * LANES : (b + 1) * LANES].astype(F32)
        for s in range(8):
            turned = pltpu.roll(block, s * PAIRS, 1) if s else block
            copies[s * 16 + b] = turned.astype(BF16)


def halves_stacked(coef):
    return jnp.concatenate([coef[:, :LANES], coef[:, LANES:]], axis=0)


def index_copy(near, scalars, sem):
    return pltpu.make_async_copy(near, scalars, sem.at[0])


def pack_kernel(fetched, other, out, near, coef, own_copies, other_copies, slots, scalars, sem):
    c = fetched[32:33, :FINE].astype(jnp.int32)
    slots[...] = ((iota((1, FINE), 1) % POINTS - c) & 7) * 16 + (c >> 3)
    fetch = index_copy(slots, scalars, sem)
    fetch.start()
    near[...] = c
    coef[...] = halves_stacked(fetched[40:44, : 2 * LANES]).astype(BF16)
    kc = lax.axis_index("kc")
    core = lax.axis_index("kf_2")
    turn_rows(fetched, own_copies)
    turn_rows(other, other_copies)
    copies = (own_copies, other_copies)
    fetch.wait()
    group = iota((PAIRS, LANES), 1) // PAIRS
    base = 16 * core + 4 * kc

    def body(d, carry):
        tiles = [None, None]
        for j in range(POINTS):
            slot = scalars[0, 32 * d + base + j]
            for lo in range(2):
                for n in range(2):
                    piece = copies[n][slot ^ (64 * lo), lo * PAIRS : (lo + 1) * PAIRS, :]
                    tiles[n] = piece if tiles[n] is None else jnp.where(group == lo * POINTS + j, piece, tiles[n])
        out[d, pl.ds(pl.multiple_of(core * PAIRS, PAIRS), PAIRS), :] = tiles[0]
        out[d, pl.ds(pl.multiple_of((1 - core) * PAIRS, PAIRS), PAIRS), :] = tiles[1]
        out[d, 2 * PAIRS :, :] = coef[...]
        return carry

    lax.fori_loop(0, PEERS, body, 0, unroll=4)


def row_block(received, n):
    return received[n // 2, n % 2 * PAIRS : (n % 2 + 1) * PAIRS, :]


def row_coefficients(coef_own):
    mine = coef_own[...].astype(F32)
    return jnp.concatenate([mine, mine], axis=0).astype(BF16)


def put_pieces(received, kc, target, at):
    for p in range(8):
        target[at + p // 2, p % 2 * 8 : p % 2 * 8 + 8, :] = received[kc * 8 + p, 2 * PAIRS :, :]


def split_kernel(received, coef_own, up_1, up_2, down_1, down_2, across):
    kc = lax.axis_index("kc")
    mine = row_coefficients(coef_own)
    for n in range(64):
        block = row_block(received, n)
        if n < RISING:
            up_1[n] = block
            down_2[n] = block
        else:
            up_2[n - RISING] = block
            down_1[n - RISING] = block
    for step, target, at in ((1, up_1, RISING), (3, down_1, 64 - RISING), (2, across, 0)):
        put_pieces(received, (kc + step) % 4, target, at)
        target[at + 4] = mine


def collect_kernel(received, left_1, right_1, far_coef, collected):
    put_pieces(received, lax.axis_index("kc"), collected, 0)
    for n in range(4):
        collected[4 + n] = left_1[RISING + n]
        collected[8 + n] = right_1[64 - RISING + n]
        collected[12 + n] = far_coef[n]


def spread(row_of, count):
    keep = iota((8, LANES), 1) // PAIRS == iota((8, LANES), 0)
    pieces = []
    for p in range(count):
        for half in range(2):
            pieces.append(jnp.where(keep, jnp.broadcast_to(row_of(p, half), (8, LANES)), 0.0))
    return jnp.concatenate(pieces, axis=0).astype(BF16)


def repeat_matrix():
    same = iota((LANES, LANES), 0) % PAIRS == iota((LANES, LANES), 1) % PAIRS
    return jnp.where(same, 1.0, 0.0).astype(BF16)


def pair_blocks(low_of, high_of, pairs):
    low = iota((PAIRS, LANES), 1) < 64
    for n in range(64):
        first, second = low_of(n), high_of(n)
        pairs[2 * n] = jnp.where(low, first, pltpu.roll(second.astype(F32), 64, 1).astype(BF16))
        pairs[2 * n + 1] = jnp.where(low, pltpu.roll(first.astype(F32), 64, 1).astype(BF16), second)


def turn_points(scalars, first, pairs, turn, picked, turned, v):
    for i in range(64):
        picked[v % 2, i * PAIRS : (i + 1) * PAIRS, :] = pairs[scalars[0, first + 64 * v + i]]
    turned[:, v * 1024 : (v + 1) * 1024] = dot_t(turn, picked[v % 2]).astype(BF16)


def expand_points(turned, cols, result, v):
    for u in range(8 * v, 8 * v + 8):
        at = slice(u * LANES, (u + 1) * LANES)
        result[:, at] = jnp.dot(turned[:, at], cols[u], preferred_element_type=F32).astype(BF16)


def row_copy(result, out, sem, n, step, v):
    row = pl.multiple_of((lax.axis_index("kc") + step) % 4 * 64, 64)
    at = pl.ds(v * 1024, 1024)
    return pltpu.make_async_copy(result.at[pl.ds(n % 2 * 64, 64), at], out.at[pl.ds(row, 64), at], sem.at[1 + 4 * n + v])


def diagonal():
    same = iota((LANES, LANES), 0) // PAIRS == iota((LANES, LANES), 1) // PAIRS
    return jnp.where(same, 1.0, 0.0).astype(BF16)


def turn_of(first, second, repeat, diag):
    rows = (first.astype(F32), second.astype(F32))

    def row_of(p, half):
        at = half * POINTS + p % POINTS
        return rows[p // POINTS][at : at + 1]

    return jnp.dot(spread(row_of, 8), repeat, preferred_element_type=F32).astype(BF16) * diag


def turn_kernel(near, received, coef_own, left_1, left_2, turned, pairs, picked, scalars, sem):
    fetch = index_copy(near, scalars, sem)
    fetch.start()
    kc = lax.axis_index("kc")
    turn = turn_of(coef_own[...], left_1[RISING + 4], repeat_matrix(), diagonal())
    pair_blocks(
        lambda n: row_block(received, n), lambda n: left_1[n] if n < RISING else left_2[n - RISING], pairs
    )
    fetch.wait()
    for v in range(4):
        turn_points(scalars, 256 * kc, pairs, turn, picked, turned, v)


def final_kernel(
    near, coef_half, coef_other, right_1, right_2, far_1, far_2, far_coef, rows_turned, out,
    pieces, cols, diag, pairs, picked, turned, first, second, scalars, sem
):
    fetch = index_copy(near, scalars, sem)
    fetch.start()
    kc = lax.axis_index("kc")
    core = lax.axis_index("kf_2")
    repeat = repeat_matrix()
    diag[...] = diagonal()
    turn = turn_of(right_1[68 - RISING], far_coef[4], repeat, diag[...])
    for n, step in enumerate((0, 3, 1, 2)):
        for p in range(8):
            for owner, source in ((core, coef_half), (1 - core, coef_other)):
                piece = source[4 * n + p // 2, p % 2 * 8 : p % 2 * 8 + 8, :].astype(F32)
                pieces[(kc + step) % 4, p, pl.ds(pl.multiple_of(owner * 8, 8), 8), :] = piece

    def build(v):
        for s in range(8):
            p_index, h, par = 2 * v + s // 4, s // 2 % 2, s % 2

            def row_of(p, half):
                r = h * 8 + half * POINTS + p % POINTS
                return pieces[par * 2 + p // POINTS, p_index, r : r + 1, :]

            cols[8 * v + s] = dot_t(repeat, spread(row_of, 8)).astype(BF16) * diag[...]

    for v in range(5):
        if v < 4:
            build(v)
        if v > 0:
            expand_points(rows_turned, cols, first, v - 1)
            for n, step in enumerate((0, 3)):
                row_copy(first, out, sem, n, step, v - 1).start()
    pair_blocks(
        lambda n: right_2[n] if n < RISING else right_1[n - RISING],
        lambda n: far_1[n] if n < RISING else far_2[n - RISING],
        pairs,
    )
    fetch.wait()
    for v in range(5):
        if v < 4:
            turn_points(scalars, 256 * kc, pairs, turn, picked, turned, v)
        if v > 0:
            expand_points(turned, cols, second, v - 1)
            for n, step in enumerate((1, 2)):
                row_copy(second, out, sem, n + 2, step, v - 1).start()
    for v in range(4):
        for n, step in enumerate((0, 3)):
            row_copy(first, out, sem, n, step, v).wait()
        for n, step in enumerate((1, 2)):
            row_copy(second, out, sem, n + 2, step, v).wait()


def call(kernel, outs, in_specs, out_specs, scratch, flops, aliases=None):
    return pl.pallas_call(
        kernel,
        out_shape=outs,
        in_specs=in_specs,
        out_specs=out_specs,
        scratch_shapes=scratch,
        input_output_aliases=aliases or {},
        compiler_params=pltpu.CompilerParams(vmem_limit_bytes=12 << 20),
        cost_estimate=pl.CostEstimate(flops=flops, bytes_accessed=flops // 10, transcendentals=0),
    )


def shape(*dims):
    return jax.ShapeDtypeStruct(dims, BF16)


def shift(value, by):
    return lax.ppermute(value, "kc", [(i, (i + by) % 4) for i in range(4)])


def partner(value):
    return lax.ppermute(value, "kf_2", [(0, 1), (1, 0)])


def shards(kernel_coarse, coefficients, nearest):
    other = partner(kernel_coarse)
    rotations = (128, 32, LANES)
    block = (PAIRS, LANES)
    table = jnp.pad(nearest.reshape(1, FINE), ((32, 15), (0, FINE))).astype(F32)
    rows = jnp.pad(coefficients.astype(F32), ((40, 4), (0, 2 * FINE - 2 * LANES)))
    fetched = jnp.pad(kernel_coarse.astype(F32), ((0, 16), (0, 0))) + table + rows
    scalars = [pltpu.SMEM((1, FINE), jnp.int32), pltpu.SemaphoreType.DMA((17,))]
    copies = pltpu.VMEM(rotations, BF16)
    packed, near, coef_own = call(
        pack_kernel,
        (shape(PEERS, 40, LANES), jax.ShapeDtypeStruct((1, FINE), jnp.int32), shape(8, LANES)),
        [VMEM] * 2,
        (VMEM,) * 3,
        [copies, copies, pltpu.VMEM((1, FINE), jnp.int32)] + scalars,
        1000000,
    )(fetched, other)
    received = lax.all_to_all(packed, ZY, split_axis=0, concat_axis=0, tiled=True)
    sizes = (RISING + 5, 64 - RISING, 69 - RISING, RISING, 5)
    up_1, up_2, down_1, down_2, across = call(
        split_kernel, tuple(shape(n, *block) for n in sizes), [VMEM] * 2, (VMEM,) * 5, [], 100000
    )(received, coef_own)
    left_1 = shift(up_1, 1)
    right_1 = shift(down_1, -1)
    far_coef = shift(across, 2)
    left_2 = shift(up_2, 1)
    right_2 = shift(down_2, -1)
    far_1 = shift(left_1[:RISING], 1)
    far_2 = shift(right_1[: 64 - RISING], -1)
    coef_half = call(collect_kernel, shape(16, *block), [VMEM] * 4, VMEM, [], 100000)(received, left_1, right_1, far_coef)
    coef_other = partner(coef_half)
    pairs = pltpu.VMEM((128, *block), BF16)
    picked = pltpu.VMEM((2, 1024, LANES), BF16)
    turned = pltpu.VMEM((LANES, 4096), BF16)
    rows_turned = call(
        turn_kernel, shape(LANES, 4096), [VMEM] * 5, VMEM, [pairs, picked] + scalars, 2000000
    )(near, received, coef_own, left_1, left_2)
    return call(
        final_kernel,
        shape(256, 4096),
        [VMEM] * 9,
        ANY,
        [
            pltpu.VMEM((4, 8, *block), F32),
            pltpu.VMEM((32, LANES, LANES), BF16),
            pltpu.VMEM((LANES, LANES), BF16),
            pairs,
            picked,
            turned,
            turned,
            turned,
        ]
        + scalars,
        8000000,
    )(near, coef_half, coef_other, right_1, right_2, far_1, far_2, far_coef, rows_turned)


def solution(mesh):
    split = Mesh(mesh.devices.reshape(8, 4, 2, mesh.shape["kc"]), KF_KC)
    return jax.shard_map(
        shards,
        mesh=split,
        in_specs=(P(KF, None), P(KF_KC, None), P()),
        out_specs=P(KF, "kc"),
        check_vma=False,
    )
```
